32 devices in a mesh: parts: 2 (over x), shot: 2 (over core), space: 8 (over z, y).
Axes of the slice: x: 2, y: 2, z: 4, core: 2. Of those that a mesh axis runs over, the one named last changes fastest.
Arguments:
- image: float32 [3200, 2, 192], P(('parts', 'space')), parts along dimension 0, may hold values from -6 to 6
- coil_maps: bfloat16 [16, 3200, 2, 192], P(None, ('parts', 'space')), parts along dimension 1, may hold values from -1.5 to 1.5
- psf_phase: float32 [3200, 576], P(('parts', 'space')), parts along dimension 0, may hold values from -3.140625 to 3.140625
- line_mask: int32 [4, 200], P(('parts', 'shot')), parts along dimension 0, may hold values 0 or 1
- motion: int32 [4, 3], P(('parts', 'shot')), parts along dimension 0, may hold values from 0 to 16
Outputs:
- result: float32 [3200, 2, 192], P(('parts', 'space')), parts along dimension 0
The draws below stay inside these ranges and needn't reach their ends.
There are 2 independent parts, one for each index of `parts`. The reference program is written for one: setup_inputs(seed, part) draws one part's arguments, and reference() takes and returns one part's arrays. A program takes and returns all parts, laid end to end along the dimension named above; each array names one. Nothing has to cross between parts.
Inputs may be any that keep to these rules, and one draw needn't show every extreme that they name: `motion`: column 0 selects the rotation angle, columns 1 and 2 the shifts along x and y.
All inputs are finite; a program needn't handle non-finite values. No bound on the sum of `line_mask` on one device may be relied on, other than what follows from the above.
Results may differ from the reference program's by a relative error of at most 0.003.
Values may be sent and summed in bfloat16 or wider, within the bound.
A program may use at most 64 MiB of HBM per device.

```python
import jax
import jax.numpy as jnp
from jax import lax

NX = 192
NY = 200
COILS = 16
Z = 8
LEVELS = 17
NR = 576
SHOTS = 2


def place_ends(entries, key, smallest, high):
    spot = [jax.random.randint(jax.random.fold_in(key, axis), (), 0, length) for axis, length in enumerate(entries.shape)]
    widest = entries.shape.index(max(entries.shape))
    beside = spot[:widest] + [(spot[widest] + 1) % entries.shape[widest]] + spot[widest + 1:]
    return entries.at[tuple(spot)].set(smallest).at[tuple(beside)].set(high)


def level_of(own_key, shape, split, smallest, top_value):
    def one(axis_at, blocks):
        heights = jax.random.uniform(jax.random.fold_in(jax.random.fold_in(own_key, 6), axis_at), (blocks,), jnp.float32, smallest / len(split), top_value / len(split))
        return jnp.repeat(jnp.exp(heights), shape[axis_at] // blocks).reshape((-1,) + (1,) * (len(shape) - axis_at - 1))

    factor_of = one(*split[0])
    for cut in split[1:]:
        factor_of = factor_of * one(*cut)
    return factor_of


def scatter_about(key, extent, deviation, most, cuts=(), held_as=jnp.bfloat16):
    entries = deviation * jax.random.normal(key, extent, jnp.float32)
    if cuts:
        entries = entries * level_of(key, extent, cuts, -0.22, 0.18)
    return jnp.clip(entries, -most, most).astype(held_as)


def setup_inputs(seed: int = 0, part: int = 0) -> dict:
    splits = jax.random.split(jax.random.key(seed), 6)
    own_keys = jax.random.split(jax.random.fold_in(splits[5], part), 6)
    image = scatter_about(own_keys[0], (Z * NY, 2, NX), 1.0, 6.0, ((0, 8),), jnp.float32)
    coil_maps = scatter_about(own_keys[1], (COILS, Z * NY, 2, NX), COILS ** -0.5, 1.5, ((1, 8),))
    psf_phase = jnp.clip(jax.random.uniform(own_keys[2], (Z * NY, NR), jnp.float32, -3.140625, 3.140625), -3.140625, 3.140625)
    line_mask = place_ends((jax.random.randint(own_keys[3], (SHOTS, NY), 0, 3) < 1).astype(jnp.int32), jax.random.fold_in(own_keys[3], 1), 0, 1)
    motion = place_ends(jax.random.randint(own_keys[4], (SHOTS, 3), 0, LEVELS), jax.random.fold_in(own_keys[4], 1), 0, LEVELS - 1).astype(jnp.int32)
    return dict(image=image, coil_maps=coil_maps, psf_phase=psf_phase, line_mask=line_mask, motion=motion)


PRECISE = lax.Precision.HIGHEST
ANGLE_STEP = 0.02
SHIFT_STEP = 0.5


def dft_parts(size_in, size_out, modulus, sign):
    inputs = jnp.arange(size_in, dtype=jnp.int32)[:, None]
    outputs = jnp.arange(size_out, dtype=jnp.int32)[None, :]
    angle = ((inputs * outputs) % modulus).astype(jnp.float32) * (2.0 * jnp.pi / modulus)
    factor = float(modulus) ** -0.5
    return jnp.cos(angle) * factor, jnp.sin(angle) * (sign * factor)


def block(parts):
    real_part, imag_part = parts
    upper = jnp.concatenate([real_part, imag_part], 1)
    bottom = jnp.concatenate([-imag_part, real_part], 1)
    return jnp.concatenate([upper, bottom], 0)


def quad(real_part, imag_part):
    return jnp.stack([jnp.stack([real_part, -imag_part], 1), jnp.stack([imag_part, real_part], 1)], 0)


def signed_freq(length):
    counter = jnp.arange(length, dtype=jnp.int32)
    return jnp.where(counter < length // 2, counter, counter - length).astype(jnp.float32)


def turn_phase(values, phase):
    cosine = jnp.cos(phase)
    sine_part = jnp.sin(phase)
    real_part = values[..., 0, :]
    imag_part = values[..., 1, :]
    return jnp.stack([real_part * cosine - imag_part * sine_part, real_part * sine_part + imag_part * cosine], -2)


def complex_mul(left, right):
    return jnp.stack([left[..., 0, :] * right[..., 0, :] - left[..., 1, :] * right[..., 1, :],
                      left[..., 0, :] * right[..., 1, :] + left[..., 1, :] * right[..., 0, :]], -2)


def conj_mul(left, right):
    return jnp.stack([left[..., 0, :] * right[..., 0, :] + left[..., 1, :] * right[..., 1, :],
                      left[..., 0, :] * right[..., 1, :] - left[..., 1, :] * right[..., 0, :]], -2)


def shear_rows(values, shift, sign):
    length = values.shape[-1]
    lines = values.shape[0]
    forward = block(dft_parts(length, length, length, -1.0))
    inverse = block(dft_parts(length, length, length, 1.0))
    spectra = jnp.dot(values.reshape(lines, 2 * length), forward, precision=PRECISE, preferred_element_type=jnp.float32)
    phase = (sign * -2.0 * jnp.pi / length) * shift[:, None] * signed_freq(length)[None, :]
    spectra = turn_phase(spectra.reshape(lines, 2, length), phase)
    result = jnp.dot(spectra.reshape(lines, 2 * length), inverse, precision=PRECISE, preferred_element_type=jnp.float32)
    return result.reshape(lines, 2, length)


def shear_columns(values, shift, sign):
    length = values.shape[1]
    forward = quad(*dft_parts(length, length, length, -1.0))
    inverse = quad(*dft_parts(length, length, length, 1.0))
    spectra = jnp.einsum("oaib,zbix->zaox", forward, values, precision=PRECISE)
    phase = (sign * -2.0 * jnp.pi / length) * signed_freq(length)[:, None] * shift[None, :]
    spectra = turn_phase(spectra, phase)
    return jnp.einsum("oaib,zbix->zaox", inverse, spectra, precision=PRECISE)


def geometry(motion_row):
    offsets = motion_row.astype(jnp.float32) - (LEVELS - 1) / 2.0
    angle = offsets[0] * ANGLE_STEP
    return -jnp.tan(angle / 2.0), jnp.sin(angle), offsets[1] * SHIFT_STEP, offsets[2] * SHIFT_STEP


def rotate(values, motion_row, sign):
    slope, tilt, shift_x, shift_y = geometry(motion_row)
    lines = values.shape[0]
    width = values.shape[2]
    across = (jnp.arange(lines, dtype=jnp.int32) % NY).astype(jnp.float32) - NY / 2.0
    along = jnp.arange(width, dtype=jnp.int32).astype(jnp.float32) - width / 2.0

    def column_pass(current):
        view_slices = current.reshape(lines // NY, NY, 2, width)
        return shear_columns(view_slices, tilt * along + shift_y, sign).reshape(lines, 2, width)

    if sign > 0:
        current = shear_rows(values, slope * across + shift_x, 1.0)
        current = column_pass(current)
        return shear_rows(current, slope * across, 1.0)
    current = shear_rows(values, slope * across, -1.0)
    current = column_pass(current)
    return shear_rows(current, slope * across + shift_x, -1.0)


def line_table(mask_row):
    cosine, sine_part = dft_parts(NY, NY, NY, 1.0)
    weight = mask_row.astype(jnp.float32)[:, None]
    real_part = jnp.dot(cosine.T, weight * cosine, precision=PRECISE) + jnp.dot(sine_part.T, weight * sine_part, precision=PRECISE)
    imag_part = jnp.dot(sine_part.T, weight * cosine, precision=PRECISE) - jnp.dot(cosine.T, weight * sine_part, precision=PRECISE)
    return quad(real_part, imag_part).astype(jnp.bfloat16)


def reference(image, coil_maps, psf_phase, line_mask, motion):
    lines = image.shape[0]
    width = image.shape[2]
    readout = psf_phase.shape[1]
    pad_table = block(dft_parts(width, readout, readout, -1.0)).astype(jnp.bfloat16)
    crop_table = block(dft_parts(readout, width, readout, 1.0)).astype(jnp.bfloat16)

    def one_shot(running, inputs):
        mask_row, motion_row = inputs
        projector = line_table(mask_row).astype(jnp.float32)
        rotated = rotate(image, motion_row, 1)

        def one_coil(combined, coil):
            coil_values = coil.astype(jnp.float32)
            coil_image = complex_mul(coil_values, rotated).astype(jnp.bfloat16)
            spectra = jnp.dot(coil_image.reshape(lines, 2 * width), pad_table, preferred_element_type=jnp.float32)
            waved = turn_phase(spectra.reshape(lines, 2, readout), psf_phase).astype(jnp.bfloat16)
            view_slices = waved.reshape(lines // NY, NY, 2, readout).astype(jnp.float32)
            projected = jnp.einsum("oaib,zbik->zaok", projector, view_slices, precision=PRECISE).astype(jnp.bfloat16)
            unwaved = turn_phase(projected.reshape(lines, 2, readout).astype(jnp.float32), -psf_phase).astype(jnp.bfloat16)
            back = jnp.dot(unwaved.reshape(lines, 2 * readout), crop_table, preferred_element_type=jnp.float32)
            return combined + conj_mul(coil_values, back.reshape(lines, 2, width)), None

        combined, _ = lax.scan(one_coil, jnp.zeros(image.shape, jnp.float32), coil_maps)
        return running + rotate(combined, motion_row, -1), None

    result, _ = lax.scan(one_shot, jnp.zeros(image.shape, jnp.float32), (line_mask, motion))
    return result
```

```python
import functools
import math

import jax
import jax.numpy as jnp
import numpy as np
from jax import lax
from jax.experimental import pallas as pl
from jax.experimental.pallas import tpu as pltpu
from jax.sharding import PartitionSpec as P

NY = 200
LEVELS = 17


PRECISE = lax.Precision.HIGHEST
ANGLE_STEP = 0.02
SHIFT_STEP = 0.5


def from_partner(value, axis, apart):
    mask = 2**apart
    pairs = [(source, source ^ mask) for source in range(lax.axis_size(axis))]
    return lax.ppermute(value, axis, pairs)


def dft_parts(size_in, size_out, modulus, sign):
    inputs = jnp.arange(size_in, dtype=jnp.int32)[:, None]
    outputs = jnp.arange(size_out, dtype=jnp.int32)[None, :]
    angle = (inputs * outputs % modulus).astype(jnp.float32) * (2.0 * jnp.pi / modulus)
    factor = float(modulus) ** (-0.5)
    return (jnp.cos(angle) * factor, jnp.sin(angle) * (sign * factor))


def block(parts):
    real_part, imag_part = parts
    upper = jnp.concatenate([real_part, imag_part], 1)
    bottom = jnp.concatenate([-imag_part, real_part], 1)
    return jnp.concatenate([upper, bottom], 0)


def quad(real_part, imag_part):
    return jnp.stack(
        [jnp.stack([real_part, -imag_part], 1), jnp.stack([imag_part, real_part], 1)], 0
    )


def signed_freq(length):
    counter = jnp.arange(length, dtype=jnp.int32)
    return jnp.where(counter < length // 2, counter, counter - length).astype(jnp.float32)


def turn_phase(values, phase):
    cosine = jnp.cos(phase)
    sine_part = jnp.sin(phase)
    real_part = values[..., 0, :]
    imag_part = values[..., 1, :]
    return jnp.stack(
        [real_part * cosine - imag_part * sine_part, real_part * sine_part + imag_part * cosine], -2
    )


def complex_mul(left, right):
    return jnp.stack(
        [
            left[..., 0, :] * right[..., 0, :] - left[..., 1, :] * right[..., 1, :],
            left[..., 0, :] * right[..., 1, :] + left[..., 1, :] * right[..., 0, :],
        ],
        -2,
    )


def conj_mul(left, right):
    return jnp.stack(
        [
            left[..., 0, :] * right[..., 0, :] + left[..., 1, :] * right[..., 1, :],
            left[..., 0, :] * right[..., 1, :] - left[..., 1, :] * right[..., 0, :],
        ],
        -2,
    )


def shear_rows(values, shift, sign):
    length = values.shape[-1]
    lines = values.shape[0]
    forward = block(dft_parts(length, length, length, -1.0))
    inverse = block(dft_parts(length, length, length, 1.0))
    spectra = jnp.dot(
        values.reshape(lines, 2 * length),
        forward,
        precision=PRECISE,
        preferred_element_type=jnp.float32,
    )
    phase = sign * -2.0 * jnp.pi / length * shift[:, None] * signed_freq(length)[None, :]
    spectra = turn_phase(spectra.reshape(lines, 2, length), phase)
    result = jnp.dot(
        spectra.reshape(lines, 2 * length),
        inverse,
        precision=PRECISE,
        preferred_element_type=jnp.float32,
    )
    return result.reshape(lines, 2, length)


def shear_columns(values, shift, sign):
    length = values.shape[1]
    forward = quad(*dft_parts(length, length, length, -1.0))
    inverse = quad(*dft_parts(length, length, length, 1.0))
    spectra = jnp.einsum("oaib,zbix->zaox", forward, values, precision=PRECISE)
    phase = sign * -2.0 * jnp.pi / length * signed_freq(length)[:, None] * shift[None, :]
    spectra = turn_phase(spectra, phase)
    return jnp.einsum("oaib,zbix->zaox", inverse, spectra, precision=PRECISE)


def geometry(motion_row):
    offsets = motion_row.astype(jnp.float32) - (LEVELS - 1) / 2.0
    angle = offsets[0] * ANGLE_STEP
    return (-jnp.tan(angle / 2.0), jnp.sin(angle), offsets[1] * SHIFT_STEP, offsets[2] * SHIFT_STEP)


def line_table(mask_row):
    cosine, sine_part = dft_parts(NY, NY, NY, 1.0)
    weight = mask_row.astype(jnp.float32)[:, None]
    real_part = jnp.dot(cosine.T, weight * cosine, precision=PRECISE) + jnp.dot(
        sine_part.T, weight * sine_part, precision=PRECISE
    )
    imag_part = jnp.dot(sine_part.T, weight * cosine, precision=PRECISE) - jnp.dot(
        cosine.T, weight * sine_part, precision=PRECISE
    )
    return quad(real_part, imag_part).astype(jnp.bfloat16)


def to_columns(values):
    return lax.all_to_all(values, "space", split_axis=2, concat_axis=0, tiled=True)


def to_rows(values):
    return lax.all_to_all(values, "space", split_axis=0, concat_axis=2, tiled=True)


def rotate_shards(values, motion_row, sign, device_rank, devices):
    slope, tilt, shift_x, shift_y = geometry(motion_row)
    lines = values.shape[0]
    width = values.shape[2]
    across = ((device_rank * lines + jnp.arange(lines, dtype=jnp.int32)) % NY).astype(
        jnp.float32
    ) - NY / 2.0

    def column_pass(current):
        columns = width // devices
        along = (device_rank * columns + jnp.arange(columns, dtype=jnp.int32)).astype(
            jnp.float32
        ) - width / 2.0
        gathered = to_columns(current)
        all_lines = gathered.shape[0]
        view_slices = gathered.reshape(all_lines // NY, NY, 2, columns)
        sheared = shear_columns(view_slices, tilt * along + shift_y, sign).reshape(
            all_lines, 2, columns
        )
        return to_rows(sheared)

    if sign > 0:
        current = shear_rows(values, slope * across + shift_x, 1.0)
        current = column_pass(current)
        return shear_rows(current, slope * across, 1.0)
    current = shear_rows(values, slope * across, -1.0)
    current = column_pass(current)
    return shear_rows(current, slope * across + shift_x, -1.0)


def gather_slice(values, bit_count, device_rank):
    for bit_index in range(bit_count):
        partner = from_partner(values, "space", bit_index)
        low_side = device_rank >> bit_index & 1 == 0
        values = jnp.where(
            low_side, jnp.concatenate([values, partner], 0), jnp.concatenate([partner, values], 0)
        )
    return values


def sum_slice(values, bit_count, device_rank):
    for bit_index in reversed(range(bit_count)):
        half_rows = values.shape[0] // 2
        low_side = device_rank >> bit_index & 1 == 0
        kept_part = jnp.where(low_side, values[:half_rows], values[half_rows:])
        sent_part = jnp.where(low_side, values[half_rows:], values[:half_rows])
        values = kept_part + from_partner(sent_part, "space", bit_index)
    return values


def regroup_coils(coil_maps, bit_count, device_rank):
    group_size = 1 << bit_count
    pieces = coil_maps.reshape((group_size, coil_maps.shape[0] // group_size) + coil_maps.shape[1:])
    for bit_index in range(bit_count):
        old_shape = pieces.shape
        halves = pieces.reshape((group_size >> bit_index + 1, 2, 1 << bit_index) + old_shape[1:])
        low_side = device_rank >> bit_index & 1 == 0
        kept_part = jnp.where(low_side, halves[:, 0], halves[:, 1])
        sent_part = jnp.where(low_side, halves[:, 1], halves[:, 0])
        partner = from_partner(sent_part, "space", bit_index)
        pieces = jnp.stack(
            [jnp.where(low_side, kept_part, partner), jnp.where(low_side, partner, kept_part)], 1
        ).reshape(old_shape)
    moved = jnp.moveaxis(pieces, 0, 1)
    return moved.reshape((moved.shape[0], group_size * coil_maps.shape[1]) + coil_maps.shape[2:])


def encode(coils, slab_image, psf_values, pad_table):
    coil_count, lines, _, width = coils.shape
    readout = psf_values.shape[1]
    coil_image = complex_mul(coils.astype(jnp.float32), slab_image[None]).astype(jnp.bfloat16)
    spectra = jnp.dot(
        coil_image.reshape(coil_count * lines, 2 * width),
        pad_table,
        preferred_element_type=jnp.float32,
    )
    return turn_phase(spectra.reshape(coil_count, lines, 2, readout), psf_values[None]).astype(
        jnp.bfloat16
    )


def project(projector, waved):
    coil_count, lines, _, columns = waved.shape
    view_slices = waved.reshape(coil_count, lines // NY, NY, 2, columns)
    projected = jnp.einsum(
        "oaib,czbik->czaok", projector, view_slices, preferred_element_type=jnp.float32
    )
    return projected.astype(jnp.bfloat16).reshape(waved.shape)


def decode(coils, projected, psf_values, crop_table):
    coil_count, lines, _, readout = projected.shape
    width = coils.shape[3]
    unwaved = turn_phase(projected.astype(jnp.float32), -psf_values[None]).astype(jnp.bfloat16)
    back = jnp.dot(
        unwaved.reshape(coil_count * lines, 2 * readout),
        crop_table,
        preferred_element_type=jnp.float32,
    )
    return jnp.sum(
        conj_mul(coils.astype(jnp.float32), back.reshape(coil_count, lines, 2, width)), 0
    )


def round_up(size, step):
    return -(-size // step) * step


HALF = 128
TALL = 2 * HALF


def fits(height, width, readout):
    return (
        height % 2 == 0
        and HALF < height
        and height // 2 < HALF
        and width % 32 == 0
        and width <= TALL
        and readout % 32 == 0
    )


def cosine_sine(rows, columns, modulus):
    turns = np.outer(rows, columns) % modulus
    angle = turns.astype(np.float64) * (2.0 * np.pi / modulus)
    return np.cos(angle), np.sin(angle)


def half_spectrum(points, modulus):
    half = modulus // 2
    cosine, sine = cosine_sine(np.arange(half), points, modulus)
    sine[0] = cosine_sine([half], points, modulus)[0][0]
    return np.concatenate([cosine, sine], 0)


def split_table(table):
    high = table.astype(np.float32).astype(jnp.bfloat16)
    low = (table - high.astype(np.float64)).astype(np.float32).astype(jnp.bfloat16)
    return np.stack([high, low])


def host_tables(width, height, readout):
    spectrum = half_spectrum(np.arange(width), readout) * readout**-0.5
    weight = np.full((width, 1), (2.0 / width) ** 0.5)
    weight[0] = weight[width // 2] = width**-0.5
    row = half_spectrum(np.arange(width), width) * weight

    middle = height // 2
    lines = np.arange(height)
    spread = np.where(lines < middle, lines, lines - middle + HALF)
    cosine, sine = cosine_sine(lines, np.arange(middle + 1), height)
    wave = np.zeros((height, TALL))
    wave[:, : middle + 1] = cosine * (2.0 / height) ** 0.5
    wave[:, 0] = height**-0.5
    wave[:, middle] = cosine[:, middle] * height**-0.5
    wave[:, HALF + 1 : HALF + middle] = sine[:, 1:middle] * (2.0 / height) ** 0.5
    natural = np.zeros((TALL, TALL))
    natural[:height] = wave
    padded = np.zeros((TALL, TALL))
    padded[spread] = wave

    cosine, sine = [part * height**-0.5 for part in cosine_sine(lines, lines, height)]
    line_left = np.zeros((HALF, 2 * TALL))
    line_left[:middle, :height] = cosine[:middle]
    line_left[:middle, TALL : TALL + height] = sine[:middle]
    line_right = np.zeros((2 * TALL, TALL))
    line_right[:height, :middle] = cosine[:, :middle]
    line_right[TALL : TALL + height, :middle] = sine[:, :middle]
    line_right[:height, HALF : HALF + middle] = sine[:, :middle]
    line_right[TALL : TALL + height, HALF : HALF + middle] = -cosine[:, :middle]

    spreader = np.zeros((TALL, TALL))
    spreader[lines, spread] = 1.0
    mirror = np.zeros((readout // 2, readout // 2))
    mirror[np.arange(readout // 2), -np.arange(readout // 2) % (readout // 2)] = 1.0

    def narrow(table):
        return table.astype(np.float32).astype(jnp.bfloat16)

    return dict(
        row=split_table(row),
        row_back=split_table(row.T),
        column=split_table(natural),
        column_spread_back=split_table(padded.T),
        column_spread=split_table(padded),
        column_back=split_table(natural.T),
        spreader=narrow(spreader),
        mirror=narrow(mirror),
        line_left=split_table(line_left),
        line_right=split_table(line_right),
        encode=narrow(spectrum),
        decode=narrow(spectrum.T),
    )


SINE = [(-1.0) ** n / math.factorial(2 * n + 1) for n in range(6)]
COSINE = [(-1.0) ** n / math.factorial(2 * n) for n in range(7)]


def poly(square, coefficients):
    value = jnp.full_like(square, coefficients[-1])
    for coefficient in reversed(coefficients[:-1]):
        value = value * square + coefficient
    return value


def cos_sin_of_half(half):
    square = half * half
    sine = half * poly(square, SINE)
    cosine = poly(square, COSINE)
    return 1.0 - 2.0 * sine * sine, 2.0 * sine * cosine


def cos_sin_turns(turns):
    rest = turns - jnp.floor(turns + 0.5)
    return cos_sin_of_half(rest * math.pi)


def split_value(value):
    high = value.astype(jnp.bfloat16)
    return high, (value - high.astype(jnp.float32)).astype(jnp.bfloat16)


def mxu(left, right):
    return jnp.dot(left, right, preferred_element_type=jnp.float32)


def mxu_split(left, right):
    return mxu(left[0], right[0]) + (mxu(left[0], right[1]) + mxu(left[1], right[0]))


LOADS = (
    "image",
    "row",
    "row_back",
    "psf",
    "column",
    "column_spread_back",
    "spreader",
    "mirror",
    "line_left",
    "line_right",
    "coil",
    "encode",
    "decode",
    "column_spread",
    "column_back",
)
UNROLL = 4
SPLIT = 2


def slice_kernel(motion_ref, mask_ref, *refs):
    count = len(LOADS)
    sources = dict(zip(LOADS, refs[:count]))
    out_ref = refs[count]
    held = dict(zip(LOADS, refs[count + 1 : 2 * count + 1]))
    (
        image_s,
        psf_s,
        tail_s,
        coil_s,
        mask_s,
        table_s,
        turn_s,
        row_phase_s,
        edge_phase_s,
        column_phase_s,
        rotated_s,
        coil_image_s,
        fold_s,
        unwaved_s,
        sum_s,
        other_s,
        load_sems,
        link_sems,
    ) = refs[2 * count + 1 :]
    _, width, height = sources["image"].shape
    readout = sources["psf"].shape[0]
    coils = sources["coil"].shape[0]
    half_width, half_readout = width // 2, readout // 2
    tail = height - HALF
    ahead = HALF - height // 2

    copies = {
        name: pltpu.make_async_copy(sources[name], held[name], load_sems.at[at])
        for at, name in enumerate(LOADS)
    }
    for name in LOADS:
        copies[name].start()
    partner = {"shot": 1 - lax.axis_index("shot")}
    barrier = pltpu.get_barrier_semaphore()
    pl.semaphore_signal(
        barrier, inc=1, device_id=partner, device_id_type=pl.DeviceIdType.MESH
    )

    theta = (motion_ref[0, 0].astype(jnp.float32) - (LEVELS - 1) / 2.0) * ANGLE_STEP
    shift_x = (motion_ref[0, 1].astype(jnp.float32) - (LEVELS - 1) / 2.0) * SHIFT_STEP
    shift_y = (motion_ref[0, 2].astype(jnp.float32) - (LEVELS - 1) / 2.0) * SHIFT_STEP
    half = theta * 0.5
    half_square = half * half
    slope = -half * (
        1.0
        + half_square
        * (1.0 / 3.0 + half_square * (2.0 / 15.0 + half_square * (17.0 / 315.0)))
    )
    square = theta * theta
    tilt = theta * (
        1.0 - square * (1.0 / 6.0 - square * (1.0 / 120.0 - square * (1.0 / 5040.0)))
    )

    def iota(shape, axis):
        return lax.broadcasted_iota(jnp.int32, shape, axis)

    def floats(value):
        return value.astype(jnp.float32)

    def row_phase(slot, padded, shift):
        lane = iota((8, TALL), 1)
        line = jnp.where(lane < HALF, lane, lane - ahead) if padded else lane
        distance = slope * (floats(line) - height / 2.0) + shift
        row = iota((8, TALL), 0)
        edge = distance * jnp.where(row == 0, 0.5, floats(row) * (1.0 / width))
        edge_phase_s[slot, 0], edge_phase_s[slot, 1] = cos_sin_turns(edge)
        for at in range(0, half_width, 8):
            turns = distance * (floats(row + at) * (1.0 / width))
            cosine, sine = cos_sin_turns(turns)
            row_phase_s[slot, 0, at : at + 8] = cosine
            row_phase_s[slot, 1, at : at + 8] = sine

    def column_phase():
        frequency = floats(iota((16, HALF), 1)) * (1.0 / height)
        row = iota((16, HALF), 0)
        for at in range(0, width, 16):
            turns = (tilt * (floats(row + at) - width / 2.0) + shift_y) * frequency
            cosine, sine = cos_sin_turns(turns)
            column_phase_s[0, at : at + 16] = cosine
            column_phase_s[1, at : at + 16] = sine

    def rows_of(table, part, span):
        return held[table][part] if span is None else held[table][part, span[0] : span[1]]

    def row_apply(table, value, span=None):
        return mxu_split((rows_of(table, 0, span), rows_of(table, 1, span)), value)

    def column_apply(table, value):
        return mxu_split(split_value(value), (held[table][0], held[table][1]))

    def turn_rows(real, imag, slot, sign):
        cosine, sine = row_phase_s[slot, 0], sign * row_phase_s[slot, 1]
        edge_cosine, edge_sine = edge_phase_s[slot, 0], sign * edge_phase_s[slot, 1]
        real = row_apply("row", split_value(real))
        imag = row_apply("row", split_value(imag))
        first = iota((8, TALL), 0) == 0
        even = [value[:half_width] for value in (real, imag)]
        odd = [value[half_width:] for value in (real, imag)]
        mixed = [
            jnp.where(first, -odd[1][:8], even[0][:8]),
            jnp.where(first, odd[0][:8], even[1][:8]),
        ]
        return [
            split_value(
                jnp.concatenate(
                    [
                        cosine * even[at] - sine * odd[at],
                        edge_sine * mixed[at] + edge_cosine * odd[at][:8],
                        sine[8:] * even[at][8:] + cosine[8:] * odd[at][8:],
                    ],
                    0,
                )
            )
            for at in range(2)
        ]

    def shear_rows(real, imag, slot, sign):
        real, imag = turn_rows(real, imag, slot, sign)
        return row_apply("row_back", real), row_apply("row_back", imag)

    def shear_columns(real, imag, tables, sign):
        cosine, sine = column_phase_s[0], sign * column_phase_s[1]
        real, imag = column_apply(tables[0], real), column_apply(tables[0], imag)
        even = [value[:, :HALF] for value in (real, imag)]
        odd = [value[:, HALF:] for value in (real, imag)]
        last = iota((width, HALF), 1) == height // 2
        mixed = [jnp.where(last, even[1], odd[0]), jnp.where(last, -even[0], odd[1])]
        out = []
        for at in range(2):
            out.append(
                jnp.concatenate(
                    [
                        cosine * even[at] - sine * mixed[at],
                        sine * even[at] + cosine * odd[at],
                    ],
                    1,
                )
            )
        return column_apply(tables[1], out[0]), column_apply(tables[1], out[1])

    image_s[...] = jnp.zeros_like(image_s)
    psf_s[:, HALF:] = jnp.zeros((readout, TALL - HALF), jnp.float32)
    tail_s[...] = jnp.zeros_like(tail_s)
    mask_s[...] = jnp.zeros_like(mask_s)
    mask_s[:, :height] = floats(mask_ref[...])
    row_phase(0, False, shift_x)
    column_phase()
    row_phase(1, True, 0.0)
    copies["image"].wait()
    copies["row"].wait()
    copies["row_back"].wait()
    image_s[:, :, :height] = held["image"][...]
    real, imag = shear_rows(image_s[0], image_s[1], 0, 1.0)
    copies["column"].wait()
    copies["column_spread_back"].wait()
    real, imag = shear_columns(real, imag, ("column", "column_spread_back"), 1.0)

    copies["psf"].wait()
    psf_s[:, :height] = held["psf"][...]
    copies["spreader"].wait()
    copies["mirror"].wait()
    for at in range(0, readout, 32):
        turn = cos_sin_of_half(psf_s[at : at + 32] * 0.5)
        for which in range(2):
            value = mxu(turn[which].astype(jnp.bfloat16), held["spreader"][...])
            value = value.astype(jnp.bfloat16)
            for part in range(2):
                turn_s[which, part, at : at + 32] = value[:, part * HALF : (part + 1) * HALF]
    behind = jnp.concatenate(
        [turn_s[which, part, half_readout:] for which in range(2) for part in range(2)], 1
    )
    behind = mxu(held["mirror"][...], behind).astype(jnp.bfloat16)
    for at in range(4):
        turn_s[at // 2, at % 2, half_readout:] = behind[:, at * HALF : (at + 1) * HALF]

    copies["line_left"].wait()
    copies["line_right"].wait()
    mask = mask_s[...]
    mask = jnp.concatenate([mask, mask], 1)
    odd_line = iota(mask.shape, 1) % 2
    for parity in range(2):
        chosen = jnp.where(odd_line == parity, mask, 0.0)
        left = [
            (floats(held["line_left"][part]) * chosen).astype(jnp.bfloat16) for part in range(2)
        ]
        table = mxu_split(left, (held["line_right"][0], held["line_right"][1]))
        direct, crossed = table[:, :HALF], table[:, HALF:]
        table_s[parity, :HALF] = table.astype(jnp.bfloat16)
        table_s[parity, HALF:, :HALF] = (-crossed).astype(jnp.bfloat16)
        table_s[parity, HALF:, HALF:] = direct.astype(jnp.bfloat16)

    real, imag = shear_rows(real, imag, 1, 1.0)
    for part in range(2):
        rotated_s[part, 0] = real[:, part * HALF : (part + 1) * HALF]
        rotated_s[part, 1] = imag[:, part * HALF : (part + 1) * HALF]
    sum_s[...] = jnp.zeros_like(sum_s)

    copies["coil"].wait()
    copies["encode"].wait()
    copies["decode"].wait()

    def multiply(coil, slot):
        early = iota((width, HALF), 1) < ahead
        spread = []
        for at in range(2):
            low = floats(held["coil"][coil, at, :, :HALF])
            tail_s[at, :, :tail] = floats(held["coil"][coil, at, :, HALF:height])
            high = jnp.where(
                early, pltpu.roll(low, ahead, 1), pltpu.roll(tail_s[at], ahead, 1)
            )
            spread.append((low, high))
            coil_s[slot, at, 0] = low
            coil_s[slot, at, 1] = high
        for part in range(2):
            real, imag = rotated_s[part, 0], rotated_s[part, 1]
            coil_real, coil_imag = spread[0][part], spread[1][part]
            coil_image_s[part] = (coil_real * real - coil_imag * imag).astype(jnp.bfloat16)
            coil_image_s[2 + part] = (coil_real * imag + coil_imag * real).astype(jnp.bfloat16)

    def head(value):
        return value[:16]

    first = iota((16, HALF), 0) == 0

    def joined(chosen, value):
        return jnp.concatenate([jnp.where(first, chosen[:16], value[:16]), value[16:]], 0)

    def encode():
        spectra = mxu(
            held["encode"][...], jnp.concatenate([coil_image_s[at] for at in range(4)], 1)
        )
        waved = []
        for part in range(2):
            lanes = slice(part * HALF, (part + 1) * HALF)
            even_real, even_imag = spectra[:half_readout, :TALL], spectra[:half_readout, TALL:]
            odd_real, odd_imag = spectra[half_readout:, :TALL], spectra[half_readout:, TALL:]
            even_real, even_imag = even_real[:, lanes], even_imag[:, lanes]
            odd_real, odd_imag = odd_real[:, lanes], odd_imag[:, lanes]
            sides = (
                (joined(even_real, even_real + odd_imag), joined(even_imag, even_imag - odd_real)),
                (joined(odd_real, even_real - odd_imag), joined(odd_imag, even_imag + odd_real)),
            )
            for side, (real, imag) in enumerate(sides):
                real, imag = real.astype(jnp.bfloat16), imag.astype(jnp.bfloat16)
                rows = slice(side * half_readout, (side + 1) * half_readout)
                cosine, sine = turn_s[0, part, rows], turn_s[1, part, rows]
                waved.append((real * cosine - imag * sine, real * sine + imag * cosine))
        for side in range(2):
            rows = slice(side * half_readout, (side + 1) * half_readout)
            for at in range(2):
                low, high = waved[side][at], waved[2 + side][at]
                fold_s[0, at, rows] = low + high
                fold_s[1, at, rows] = low - high

    def project():
        even, odd = [
            mxu(jnp.concatenate([fold_s[at, 0], fold_s[at, 1]], 1), table_s[at])
            for at in range(2)
        ]
        for part, value in enumerate((even + odd, even - odd)):
            value = value.astype(jnp.bfloat16)
            real, imag = value[:, :HALF], value[:, HALF:]
            cosine, sine = turn_s[0, part], turn_s[1, part]
            unreal, unimag = real * cosine + imag * sine, imag * cosine - real * sine
            plus_real, minus_real = unreal[:half_readout], unreal[half_readout:]
            plus_imag, minus_imag = unimag[:half_readout], unimag[half_readout:]
            unwaved_s[part, :half_readout] = joined(plus_real, plus_real + minus_real)
            unwaved_s[2 + part, :half_readout] = joined(plus_imag, plus_imag + minus_imag)
            unwaved_s[part, half_readout:] = joined(minus_real, minus_imag - plus_imag)
            unwaved_s[2 + part, half_readout:] = joined(minus_imag, plus_real - minus_real)

    def decode(slot):
        back = mxu(held["decode"][...], jnp.concatenate([unwaved_s[at] for at in range(4)], 1))
        for part in range(2):
            real = back[:, part * HALF : (part + 1) * HALF]
            imag = back[:, TALL + part * HALF : TALL + (part + 1) * HALF]
            coil_real, coil_imag = coil_s[slot, 0, part], coil_s[slot, 1, part]
            sum_s[0, part] += coil_real * real + coil_imag * imag
            sum_s[1, part] += coil_real * imag - coil_imag * real

    multiply(0, 0)
    encode()
    multiply(1, 1)
    project()
    encode()
    multiply(2, 2)

    def step(at, carry):
        for inner in range(UNROLL):
            decode(inner)
            project()
            encode()
            multiply(at * UNROLL + inner + 3, (inner + 3) % UNROLL)
        return carry

    rounds = (coils - 3) // UNROLL
    lax.fori_loop(0, rounds, step, 0)
    for coil in range(rounds * UNROLL, coils):
        decode(coil % UNROLL)
        if coil + 1 < coils:
            project()
        if coil + 2 < coils:
            encode()
        if coil + 3 < coils:
            multiply(coil + 3, (coil + 3) % UNROLL)

    copies["column_spread"].wait()
    copies["column_back"].wait()
    real, imag = [jnp.concatenate([sum_s[at, 0], sum_s[at, 1]], 1) for at in range(2)]
    real, imag = shear_rows(real, imag, 1, -1.0)
    real, imag = shear_columns(real, imag, ("column_spread", "column_back"), -1.0)
    halves = turn_rows(real, imag, 0, -1.0)
    pl.semaphore_wait(barrier, 1)
    size = width // SPLIT
    links = []
    for at in range(SPLIT):
        span = (at * size, (at + 1) * size)
        for part in range(2):
            image_s[part, span[0] : span[1]] = row_apply("row_back", halves[part], span)
        links.append(
            pltpu.make_async_remote_copy(
                src_ref=image_s.at[:, pl.ds(span[0], size)],
                dst_ref=other_s.at[:, pl.ds(span[0], size)],
                send_sem=link_sems.at[2 * at],
                recv_sem=link_sems.at[2 * at + 1],
                device_id=partner,
                device_id_type=pl.DeviceIdType.MESH,
            )
        )
        links[at].start()
    for at in range(SPLIT):
        links[at].wait_recv()
        rows = slice(at * size, (at + 1) * size)
        out_ref[:, rows] = (image_s[:, rows] + other_s[:, rows])[:, :, :height]
    for at in range(SPLIT):
        links[at].wait_send()


def whole_slice(image, coil_maps, psf_phase, line_mask, motion):
    height, width, readout = image.shape[0], image.shape[2], psf_phase.shape[1]
    coils = coil_maps.shape[0]
    arrays = {
        name: jnp.asarray(table) for name, table in host_tables(width, height, readout).items()
    }
    arrays["image"] = jnp.transpose(image, (1, 2, 0))
    arrays["coil"] = jnp.transpose(coil_maps, (0, 2, 3, 1))
    arrays["psf"] = jnp.transpose(psf_phase)
    loads = [arrays[name] for name in LOADS]
    vmem = pl.BlockSpec(memory_space=pltpu.VMEM)
    anywhere = pl.BlockSpec(memory_space=pl.ANY)
    total = pl.pallas_call(
        slice_kernel,
        out_shape=jax.ShapeDtypeStruct((2, width, height), jnp.float32),
        in_specs=[pl.BlockSpec(memory_space=pltpu.SMEM), vmem] + [anywhere] * len(LOADS),
        out_specs=vmem,
        scratch_shapes=[pltpu.VMEM(value.shape, value.dtype) for value in loads]
        + [
            pltpu.VMEM((2, width, TALL), jnp.float32),
            pltpu.VMEM((readout, TALL), jnp.float32),
            pltpu.VMEM((2, width, HALF), jnp.float32),
            pltpu.VMEM((UNROLL, 2, 2, width, HALF), jnp.float32),
            pltpu.VMEM((1, TALL), jnp.float32),
            pltpu.VMEM((2, TALL, TALL), jnp.bfloat16),
            pltpu.VMEM((2, 2, readout, HALF), jnp.bfloat16),
            pltpu.VMEM((2, 2, width // 2, TALL), jnp.float32),
            pltpu.VMEM((2, 2, 8, TALL), jnp.float32),
            pltpu.VMEM((2, width, HALF), jnp.float32),
            pltpu.VMEM((2, 2, width, HALF), jnp.float32),
            pltpu.VMEM((4, width, HALF), jnp.bfloat16),
            pltpu.VMEM((2, 2, readout, HALF), jnp.bfloat16),
            pltpu.VMEM((4, readout, HALF), jnp.bfloat16),
            pltpu.VMEM((2, 2, width, HALF), jnp.float32),
            pltpu.VMEM((2, width, TALL), jnp.float32),
            pltpu.SemaphoreType.DMA((len(LOADS),)),
            pltpu.SemaphoreType.DMA((2 * SPLIT,)),
        ],
        compiler_params=pltpu.CompilerParams(
            vmem_limit_bytes=56 * 1024 * 1024, collective_id=0, has_side_effects=True
        ),
        name="slice_kernel",
    )(motion, line_mask, *loads)
    return jnp.transpose(total, (2, 0, 1))


def on_device(image, coil_maps, psf_phase, line_mask, motion):
    lines = image.shape[0]
    width = image.shape[2]
    readout = psf_phase.shape[1]
    if lines == NY and lax.axis_size("shot") == 2 and fits(lines, width, readout):
        return whole_slice(image, coil_maps, psf_phase, line_mask, motion)
    devices = lax.axis_size("space")
    device_rank = lax.axis_index("space")
    pad_table = block(dft_parts(width, readout, readout, -1.0)).astype(jnp.bfloat16)
    crop_table = block(dft_parts(readout, width, readout, 1.0)).astype(jnp.bfloat16)
    group_size = max(1, NY // lines)
    bit_count = group_size.bit_length() - 1
    own_coils = regroup_coils(coil_maps, bit_count, device_rank)
    own_psf = gather_slice(psf_phase, bit_count, device_rank)
    projector = line_table(line_mask[0])
    rotated = rotate_shards(image, motion[0], 1, device_rank, devices)
    slab_image = gather_slice(rotated, bit_count, device_rank)
    waved = encode(own_coils, slab_image, own_psf, pad_table)
    partial_sum = decode(own_coils, project(projector, waved), own_psf, crop_table)
    combined = sum_slice(partial_sum, bit_count, device_rank)
    running = rotate_shards(combined, motion[0], -1, device_rank, devices)
    return lax.psum(running, "shot")


def solution(mesh):
    in_specs = (
        P(("parts", "space"), None, None),
        P(None, ("parts", "space"), None, None),
        P(("parts", "space"), None),
        P(("parts", "shot"), None),
        P(("parts", "shot"), None),
    )
    out_specs = P(("parts", "space"), None, None)
    return jax.shard_map(
        on_device, mesh=mesh, in_specs=in_specs, out_specs=out_specs, check_vma=False
    )
```

```python
import functools
import math

import jax
import jax.numpy as jnp
import numpy as np
from jax import lax
from jax.experimental import pallas as pl
from jax.experimental.pallas import tpu as pltpu
from jax.sharding import PartitionSpec as P

NY = 200
LEVELS = 17


PRECISE = lax.Precision.HIGHEST
ANGLE_STEP = 0.02
SHIFT_STEP = 0.5


def from_partner(value, axis, apart):
    mask = 2**apart
    pairs = [(source, source ^ mask) for source in range(lax.axis_size(axis))]
    return lax.ppermute(value, axis, pairs)


def dft_parts(size_in, size_out, modulus, sign):
    inputs = jnp.arange(size_in, dtype=jnp.int32)[:, None]
    outputs = jnp.arange(size_out, dtype=jnp.int32)[None, :]
    angle = (inputs * outputs % modulus).astype(jnp.float32) * (2.0 * jnp.pi / modulus)
    factor = float(modulus) ** (-0.5)
    return (jnp.cos(angle) * factor, jnp.sin(angle) * (sign * factor))


def block(parts):
    real_part, imag_part = parts
    upper = jnp.concatenate([real_part, imag_part], 1)
    bottom = jnp.concatenate([-imag_part, real_part], 1)
    return jnp.concatenate([upper, bottom], 0)


def quad(real_part, imag_part):
    return jnp.stack(
        [jnp.stack([real_part, -imag_part], 1), jnp.stack([imag_part, real_part], 1)], 0
    )


def signed_freq(length):
    counter = jnp.arange(length, dtype=jnp.int32)
    return jnp.where(counter < length // 2, counter, counter - length).astype(jnp.float32)


def turn_phase(values, phase):
    cosine = jnp.cos(phase)
    sine_part = jnp.sin(phase)
    real_part = values[..., 0, :]
    imag_part = values[..., 1, :]
    return jnp.stack(
        [real_part * cosine - imag_part * sine_part, real_part * sine_part + imag_part * cosine], -2
    )


def complex_mul(left, right):
    return jnp.stack(
        [
            left[..., 0, :] * right[..., 0, :] - left[..., 1, :] * right[..., 1, :],
            left[..., 0, :] * right[..., 1, :] + left[..., 1, :] * right[..., 0, :],
        ],
        -2,
    )


def conj_mul(left, right):
    return jnp.stack(
        [
            left[..., 0, :] * right[..., 0, :] + left[..., 1, :] * right[..., 1, :],
            left[..., 0, :] * right[..., 1, :] - left[..., 1, :] * right[..., 0, :],
        ],
        -2,
    )


def shear_rows(values, shift, sign):
    length = values.shape[-1]
    lines = values.shape[0]
    forward = block(dft_parts(length, length, length, -1.0))
    inverse = block(dft_parts(length, length, length, 1.0))
    spectra = jnp.dot(
        values.reshape(lines, 2 * length),
        forward,
        precision=PRECISE,
        preferred_element_type=jnp.float32,
    )
    phase = sign * -2.0 * jnp.pi / length * shift[:, None] * signed_freq(length)[None, :]
    spectra = turn_phase(spectra.reshape(lines, 2, length), phase)
    result = jnp.dot(
        spectra.reshape(lines, 2 * length),
        inverse,
        precision=PRECISE,
        preferred_element_type=jnp.float32,
    )
    return result.reshape(lines, 2, length)


def shear_columns(values, shift, sign):
    length = values.shape[1]
    forward = quad(*dft_parts(length, length, length, -1.0))
    inverse = quad(*dft_parts(length, length, length, 1.0))
    spectra = jnp.einsum("oaib,zbix->zaox", forward, values, precision=PRECISE)
    phase = sign * -2.0 * jnp.pi / length * signed_freq(length)[:, None] * shift[None, :]
    spectra = turn_phase(spectra, phase)
    return jnp.einsum("oaib,zbix->zaox", inverse, spectra, precision=PRECISE)


def geometry(motion_row):
    offsets = motion_row.astype(jnp.float32) - (LEVELS - 1) / 2.0
    angle = offsets[0] * ANGLE_STEP
    return (-jnp.tan(angle / 2.0), jnp.sin(angle), offsets[1] * SHIFT_STEP, offsets[2] * SHIFT_STEP)


def line_table(mask_row):
    cosine, sine_part = dft_parts(NY, NY, NY, 1.0)
    weight = mask_row.astype(jnp.float32)[:, None]
    real_part = jnp.dot(cosine.T, weight * cosine, precision=PRECISE) + jnp.dot(
        sine_part.T, weight * sine_part, precision=PRECISE
    )
    imag_part = jnp.dot(sine_part.T, weight * cosine, precision=PRECISE) - jnp.dot(
        cosine.T, weight * sine_part, precision=PRECISE
    )
    return quad(real_part, imag_part).astype(jnp.bfloat16)


def to_columns(values):
    return lax.all_to_all(values, "space", split_axis=2, concat_axis=0, tiled=True)


def to_rows(values):
    return lax.all_to_all(values, "space", split_axis=0, concat_axis=2, tiled=True)


def rotate_shards(values, motion_row, sign, device_rank, devices):
    slope, tilt, shift_x, shift_y = geometry(motion_row)
    lines = values.shape[0]
    width = values.shape[2]
    across = ((device_rank * lines + jnp.arange(lines, dtype=jnp.int32)) % NY).astype(
        jnp.float32
    ) - NY / 2.0

    def column_pass(current):
        columns = width // devices
        along = (device_rank * columns + jnp.arange(columns, dtype=jnp.int32)).astype(
            jnp.float32
        ) - width / 2.0
        gathered = to_columns(current)
        all_lines = gathered.shape[0]
        view_slices = gathered.reshape(all_lines // NY, NY, 2, columns)
        sheared = shear_columns(view_slices, tilt * along + shift_y, sign).reshape(
            all_lines, 2, columns
        )
        return to_rows(sheared)

    if sign > 0:
        current = shear_rows(values, slope * across + shift_x, 1.0)
        current = column_pass(current)
        return shear_rows(current, slope * across, 1.0)
    current = shear_rows(values, slope * across, -1.0)
    current = column_pass(current)
    return shear_rows(current, slope * across + shift_x, -1.0)


def gather_slice(values, bit_count, device_rank):
    for bit_index in range(bit_count):
        partner = from_partner(values, "space", bit_index)
        low_side = device_rank >> bit_index & 1 == 0
        values = jnp.where(
            low_side, jnp.concatenate([values, partner], 0), jnp.concatenate([partner, values], 0)
        )
    return values


def sum_slice(values, bit_count, device_rank):
    for bit_index in reversed(range(bit_count)):
        half_rows = values.shape[0] // 2
        low_side = device_rank >> bit_index & 1 == 0
        kept_part = jnp.where(low_side, values[:half_rows], values[half_rows:])
        sent_part = jnp.where(low_side, values[half_rows:], values[:half_rows])
        values = kept_part + from_partner(sent_part, "space", bit_index)
    return values


def regroup_coils(coil_maps, bit_count, device_rank):
    group_size = 1 << bit_count
    pieces = coil_maps.reshape((group_size, coil_maps.shape[0] // group_size) + coil_maps.shape[1:])
    for bit_index in range(bit_count):
        old_shape = pieces.shape
        halves = pieces.reshape((group_size >> bit_index + 1, 2, 1 << bit_index) + old_shape[1:])
        low_side = device_rank >> bit_index & 1 == 0
        kept_part = jnp.where(low_side, halves[:, 0], halves[:, 1])
        sent_part = jnp.where(low_side, halves[:, 1], halves[:, 0])
        partner = from_partner(sent_part, "space", bit_index)
        pieces = jnp.stack(
            [jnp.where(low_side, kept_part, partner), jnp.where(low_side, partner, kept_part)], 1
        ).reshape(old_shape)
    moved = jnp.moveaxis(pieces, 0, 1)
    return moved.reshape((moved.shape[0], group_size * coil_maps.shape[1]) + coil_maps.shape[2:])


def encode(coils, slab_image, psf_values, pad_table):
    coil_count, lines, _, width = coils.shape
    readout = psf_values.shape[1]
    coil_image = complex_mul(coils.astype(jnp.float32), slab_image[None]).astype(jnp.bfloat16)
    spectra = jnp.dot(
        coil_image.reshape(coil_count * lines, 2 * width),
        pad_table,
        preferred_element_type=jnp.float32,
    )
    return turn_phase(spectra.reshape(coil_count, lines, 2, readout), psf_values[None]).astype(
        jnp.bfloat16
    )


def project(projector, waved):
    coil_count, lines, _, columns = waved.shape
    view_slices = waved.reshape(coil_count, lines // NY, NY, 2, columns)
    projected = jnp.einsum(
        "oaib,czbik->czaok", projector, view_slices, preferred_element_type=jnp.float32
    )
    return projected.astype(jnp.bfloat16).reshape(waved.shape)


def decode(coils, projected, psf_values, crop_table):
    coil_count, lines, _, readout = projected.shape
    width = coils.shape[3]
    unwaved = turn_phase(projected.astype(jnp.float32), -psf_values[None]).astype(jnp.bfloat16)
    back = jnp.dot(
        unwaved.reshape(coil_count * lines, 2 * readout),
        crop_table,
        preferred_element_type=jnp.float32,
    )
    return jnp.sum(
        conj_mul(coils.astype(jnp.float32), back.reshape(coil_count, lines, 2, width)), 0
    )


def round_up(size, step):
    return -(-size // step) * step


HALF = 128
TALL = 2 * HALF


def fits(height, width, readout):
    return (
        height % 2 == 0
        and HALF < height
        and height // 2 < HALF
        and width % 32 == 0
        and width <= TALL
        and readout % 32 == 0
    )


def cosine_sine(rows, columns, modulus):
    turns = np.outer(rows, columns) % modulus
    angle = turns.astype(np.float64) * (2.0 * np.pi / modulus)
    return np.cos(angle), np.sin(angle)


def half_spectrum(points, modulus):
    half = modulus // 2
    cosine, sine = cosine_sine(np.arange(half), points, modulus)
    sine[0] = cosine_sine([half], points, modulus)[0][0]
    return np.concatenate([cosine, sine], 0)


def split_table(table):
    high = table.astype(np.float32).astype(jnp.bfloat16)
    low = (table - high.astype(np.float64)).astype(np.float32).astype(jnp.bfloat16)
    return np.stack([high, low])


def host_tables(width, height, readout):
    spectrum = half_spectrum(np.arange(width), readout) * readout**-0.5
    weight = np.full((width, 1), (2.0 / width) ** 0.5)
    weight[0] = weight[width // 2] = width**-0.5
    row = half_spectrum(np.arange(width), width) * weight

    middle = height // 2
    lines = np.arange(height)
    spread = np.where(lines < middle, lines, lines - middle + HALF)
    cosine, sine = cosine_sine(lines, np.arange(middle + 1), height)
    wave = np.zeros((height, TALL))
    wave[:, : middle + 1] = cosine * (2.0 / height) ** 0.5
    wave[:, 0] = height**-0.5
    wave[:, middle] = cosine[:, middle] * height**-0.5
    wave[:, HALF + 1 : HALF + middle] = sine[:, 1:middle] * (2.0 / height) ** 0.5
    natural = np.zeros((TALL, TALL))
    natural[:height] = wave
    padded = np.zeros((TALL, TALL))
    padded[spread] = wave

    cosine, sine = [part * height**-0.5 for part in cosine_sine(lines, lines, height)]
    line_left = np.zeros((HALF, 2 * TALL))
    line_left[:middle, :height] = cosine[:middle]
    line_left[:middle, TALL : TALL + height] = sine[:middle]
    line_right = np.zeros((2 * TALL, TALL))
    line_right[:height, :middle] = cosine[:, :middle]
    line_right[TALL : TALL + height, :middle] = sine[:, :middle]
    line_right[:height, HALF : HALF + middle] = sine[:, :middle]
    line_right[TALL : TALL + height, HALF : HALF + middle] = -cosine[:, :middle]

    half = readout // 2
    at = np.arange(half)
    ahead = np.zeros((half, -(-half // HALF) * HALF))
    ahead[at, at] = 1.0
    first = half // HALF * HALF
    behind = np.zeros((half, readout - first))
    behind[at, half + -at % half - first] = 1.0

    def narrow(table):
        return table.astype(np.float32).astype(jnp.bfloat16)

    return dict(
        row=split_table(row),
        row_back=split_table(row.T),
        column=split_table(natural),
        column_spread_back=split_table(padded.T),
        column_spread=split_table(padded),
        column_back=split_table(natural.T),
        ahead=narrow(ahead),
        behind=narrow(behind),
        line_left=split_table(line_left),
        line_right=split_table(line_right),
        encode=narrow(spectrum),
        decode=narrow(spectrum.T),
    )


SINE = [(-1.0) ** n / math.factorial(2 * n + 1) for n in range(6)]
COSINE = [(-1.0) ** n / math.factorial(2 * n) for n in range(7)]


def poly(square, coefficients):
    value = jnp.full_like(square, coefficients[-1])
    for coefficient in reversed(coefficients[:-1]):
        value = value * square + coefficient
    return value


def cos_sin_of_half(half):
    square = half * half
    sine = half * poly(square, SINE)
    cosine = poly(square, COSINE)
    return 1.0 - 2.0 * sine * sine, 2.0 * sine * cosine


def cos_sin_turns(turns):
    rest = turns - jnp.floor(turns + 0.5)
    return cos_sin_of_half(rest * math.pi)


def split_value(value):
    high = value.astype(jnp.bfloat16)
    return high, (value - high.astype(jnp.float32)).astype(jnp.bfloat16)


def mxu(left, right):
    return jnp.dot(left, right, preferred_element_type=jnp.float32)


def mxu_split(left, right):
    return mxu(left[0], right[0]) + (mxu(left[0], right[1]) + mxu(left[1], right[0]))


LOADS = (
    "motion",
    "image",
    "row",
    "row_back",
    "mask",
    "psf",
    "column",
    "column_spread_back",
    "ahead",
    "behind",
    "line_left",
    "line_right",
    "coil",
    "encode",
    "decode",
    "column_spread",
    "column_back",
)
EARLY = 6
UNROLL = 4
SPLIT = 2


def slice_kernel(*refs):
    count = len(LOADS)
    sources = dict(zip(LOADS, refs[:count]))
    own_ref, other_s = refs[count : count + 2]
    held = dict(zip(LOADS, refs[count + 2 : 2 * count + 2]))
    (
        image_s,
        psf_s,
        wave_s,
        tail_s,
        coil_s,
        mask_s,
        table_s,
        turn_s,
        row_phase_s,
        edge_phase_s,
        column_phase_s,
        rotated_s,
        coil_image_s,
        fold_s,
        unwaved_s,
        sum_s,
        load_sems,
        link_sems,
    ) = refs[2 * count + 2 :]
    _, width, height = sources["image"].shape
    readout = sources["psf"].shape[1]
    coils = sources["coil"].shape[0]
    half_width, half_readout = width // 2, readout // 2
    tail = height - HALF
    ahead = HALF - height // 2

    copies = {
        name: pltpu.make_async_copy(sources[name], held[name], load_sems.at[at])
        for at, name in enumerate(LOADS)
    }
    for name in LOADS[:EARLY]:
        copies[name].start()
    partner = {"shot": 1 - lax.axis_index("shot")}
    barrier = pltpu.get_barrier_semaphore()
    pl.semaphore_signal(
        barrier, inc=1, device_id=partner, device_id_type=pl.DeviceIdType.MESH
    )

    image_s[...] = jnp.zeros_like(image_s)
    psf_s[...] = jnp.zeros_like(psf_s)
    tail_s[...] = jnp.zeros_like(tail_s)
    mask_s[...] = jnp.zeros_like(mask_s)
    sum_s[...] = jnp.zeros_like(sum_s)
    wave_s[...] = jnp.zeros_like(wave_s)
    copies["motion"].wait()
    motion_ref = held["motion"]
    theta = (motion_ref[0, 0].astype(jnp.float32) - (LEVELS - 1) / 2.0) * ANGLE_STEP
    shift_x = (motion_ref[0, 1].astype(jnp.float32) - (LEVELS - 1) / 2.0) * SHIFT_STEP
    shift_y = (motion_ref[0, 2].astype(jnp.float32) - (LEVELS - 1) / 2.0) * SHIFT_STEP
    half = theta * 0.5
    half_square = half * half
    slope = -half * (
        1.0
        + half_square
        * (1.0 / 3.0 + half_square * (2.0 / 15.0 + half_square * (17.0 / 315.0)))
    )
    square = theta * theta
    tilt = theta * (
        1.0 - square * (1.0 / 6.0 - square * (1.0 / 120.0 - square * (1.0 / 5040.0)))
    )

    def iota(shape, axis):
        return lax.broadcasted_iota(jnp.int32, shape, axis)

    def floats(value):
        return value.astype(jnp.float32)

    def row_phase(slot, padded, shift):
        lane = iota((8, TALL), 1)
        line = jnp.where(lane < HALF, lane, lane - ahead) if padded else lane
        distance = slope * (floats(line) - height / 2.0) + shift
        row = iota((8, TALL), 0)
        edge = distance * jnp.where(row == 0, 0.5, floats(row) * (1.0 / width))
        edge_phase_s[slot, 0], edge_phase_s[slot, 1] = cos_sin_turns(edge)
        for at in range(0, half_width, 8):
            turns = distance * (floats(row + at) * (1.0 / width))
            cosine, sine = cos_sin_turns(turns)
            row_phase_s[slot, 0, at : at + 8] = cosine
            row_phase_s[slot, 1, at : at + 8] = sine

    def column_phase():
        frequency = floats(iota((16, HALF), 1)) * (1.0 / height)
        row = iota((16, HALF), 0)
        for at in range(0, width, 16):
            turns = (tilt * (floats(row + at) - width / 2.0) + shift_y) * frequency
            cosine, sine = cos_sin_turns(turns)
            column_phase_s[0, at : at + 16] = cosine
            column_phase_s[1, at : at + 16] = sine

    def rows_of(table, part, span):
        return held[table][part] if span is None else held[table][part, span[0] : span[1]]

    def row_apply(table, value, span=None):
        return mxu_split((rows_of(table, 0, span), rows_of(table, 1, span)), value)

    def column_apply(table, value):
        return mxu_split(split_value(value), (held[table][0], held[table][1]))

    def turn_rows(real, imag, slot, sign):
        cosine, sine = row_phase_s[slot, 0], sign * row_phase_s[slot, 1]
        edge_cosine, edge_sine = edge_phase_s[slot, 0], sign * edge_phase_s[slot, 1]
        real = row_apply("row", split_value(real))
        imag = row_apply("row", split_value(imag))
        first = iota((8, TALL), 0) == 0
        even = [value[:half_width] for value in (real, imag)]
        odd = [value[half_width:] for value in (real, imag)]
        mixed = [
            jnp.where(first, -odd[1][:8], even[0][:8]),
            jnp.where(first, odd[0][:8], even[1][:8]),
        ]
        return [
            split_value(
                jnp.concatenate(
                    [
                        cosine * even[at] - sine * odd[at],
                        edge_sine * mixed[at] + edge_cosine * odd[at][:8],
                        sine[8:] * even[at][8:] + cosine[8:] * odd[at][8:],
                    ],
                    0,
                )
            )
            for at in range(2)
        ]

    def shear_rows(real, imag, slot, sign):
        real, imag = turn_rows(real, imag, slot, sign)
        return row_apply("row_back", real), row_apply("row_back", imag)

    def shear_columns(real, imag, tables, sign):
        cosine, sine = column_phase_s[0], sign * column_phase_s[1]
        real, imag = column_apply(tables[0], real), column_apply(tables[0], imag)
        even = [value[:, :HALF] for value in (real, imag)]
        odd = [value[:, HALF:] for value in (real, imag)]
        last = iota((width, HALF), 1) == height // 2
        mixed = [jnp.where(last, even[1], odd[0]), jnp.where(last, -even[0], odd[1])]
        out = []
        for at in range(2):
            out.append(
                jnp.concatenate(
                    [
                        cosine * even[at] - sine * mixed[at],
                        sine * even[at] + cosine * odd[at],
                    ],
                    1,
                )
            )
        return column_apply(tables[1], out[0]), column_apply(tables[1], out[1])

    row_phase(0, False, shift_x)
    copies["image"].wait()
    copies["row"].wait()
    copies["row_back"].wait()
    for name in LOADS[EARLY:]:
        copies[name].start()
    image_s[:, :, :height] = held["image"][...]
    real, imag = shear_rows(image_s[0], image_s[1], 0, 1.0)
    column_phase()
    row_phase(1, True, 0.0)
    copies["column"].wait()
    copies["column_spread_back"].wait()
    real, imag = shear_columns(real, imag, ("column", "column_spread_back"), 1.0)

    copies["psf"].wait()
    middle = height // 2
    psf_s[:middle] = held["psf"][:middle]
    psf_s[HALF : HALF + middle] = held["psf"][middle:]
    for start in (0, HALF):
        for at in range(start, start + round_up(middle, 16), 16):
            turn = cos_sin_of_half(psf_s[at : at + 16] * 0.5)
            for which in range(2):
                wave_s[which, at : at + 16] = turn[which].astype(jnp.bfloat16)
    copies["ahead"].wait()
    copies["behind"].wait()
    for side, name in enumerate(("ahead", "behind")):
        wide = held[name].shape[1]
        for which in range(2):
            if side:
                wave = wave_s[which, :, readout - wide :]
            else:
                wave = wave_s[which, :, :wide]
            value = lax.dot_general(
                held[name][...],
                wave,
                (((1,), (1,)), ((), ())),
                preferred_element_type=jnp.float32,
            ).astype(jnp.bfloat16)
            rows = slice(side * half_readout, (side + 1) * half_readout)
            for part in range(2):
                turn_s[which, part, rows] = value[:, part * HALF : (part + 1) * HALF]

    copies["mask"].wait()
    mask_s[:, :height] = floats(held["mask"][...])
    copies["line_left"].wait()
    copies["line_right"].wait()
    mask = mask_s[...]
    mask = jnp.concatenate([mask, mask], 1)
    odd_line = iota(mask.shape, 1) % 2
    direct, crossed = [], []
    for parity in range(2):
        chosen = jnp.where(odd_line == parity, mask, 0.0)
        left = [
            (floats(held["line_left"][part]) * chosen).astype(jnp.bfloat16) for part in range(2)
        ]
        table = mxu_split(left, (held["line_right"][0], held["line_right"][1]))
        direct.append(table[:, :HALF])
        crossed.append(table[:, HALF:])
    diagonal = iota((HALF, HALF), 0) == iota((HALF, HALF), 1)

    def rounded(value):
        return floats(value.astype(jnp.bfloat16))

    whole = rounded(direct[0] + direct[1])
    even = rounded(whole + direct[0]) - whole
    direct = [
        jnp.where(diagonal, even, direct[0]),
        jnp.where(diagonal, whole - even, direct[1]),
    ]
    for parity in range(2):
        table_s[parity, :HALF, :HALF] = direct[parity].astype(jnp.bfloat16)
        table_s[parity, :HALF, HALF:] = crossed[parity].astype(jnp.bfloat16)
        table_s[parity, HALF:, :HALF] = (-crossed[parity]).astype(jnp.bfloat16)
        table_s[parity, HALF:, HALF:] = direct[parity].astype(jnp.bfloat16)

    real, imag = shear_rows(real, imag, 1, 1.0)
    for part in range(2):
        rotated_s[part, 0] = real[:, part * HALF : (part + 1) * HALF]
        rotated_s[part, 1] = imag[:, part * HALF : (part + 1) * HALF]

    copies["coil"].wait()
    copies["encode"].wait()
    copies["decode"].wait()

    def multiply(coil, slot):
        early = iota((width, HALF), 1) < ahead
        spread = []
        for at in range(2):
            low = floats(held["coil"][coil, at, :, :HALF])
            tail_s[at, :, :tail] = floats(held["coil"][coil, at, :, HALF:height])
            high = jnp.where(
                early, pltpu.roll(low, ahead, 1), pltpu.roll(tail_s[at], ahead, 1)
            )
            spread.append((low, high))
            coil_s[slot, at, 0] = low
            coil_s[slot, at, 1] = high
        reals, imags = [], []
        for part in range(2):
            real, imag = rotated_s[part, 0], rotated_s[part, 1]
            coil_real, coil_imag = spread[0][part], spread[1][part]
            reals.append((coil_real * real - coil_imag * imag).astype(jnp.bfloat16))
            imags.append((coil_real * imag + coil_imag * real).astype(jnp.bfloat16))
        return reals + imags

    first = iota((16, HALF), 0) == 0

    def joined(chosen, value):
        return jnp.concatenate([jnp.where(first, chosen[:16], value[:16]), value[16:]], 0)

    def encode(coil_image):
        spectra = mxu(held["encode"][...], jnp.concatenate(coil_image, 1))
        waved = []
        for part in range(2):
            lanes = slice(part * HALF, (part + 1) * HALF)
            even_real, even_imag = spectra[:half_readout, :TALL], spectra[:half_readout, TALL:]
            odd_real, odd_imag = spectra[half_readout:, :TALL], spectra[half_readout:, TALL:]
            even_real, even_imag = even_real[:, lanes], even_imag[:, lanes]
            odd_real, odd_imag = odd_real[:, lanes], odd_imag[:, lanes]
            sides = (
                (joined(even_real, even_real + odd_imag), joined(even_imag, even_imag - odd_real)),
                (joined(odd_real, even_real - odd_imag), joined(odd_imag, even_imag + odd_real)),
            )
            for side, (real, imag) in enumerate(sides):
                real, imag = real.astype(jnp.bfloat16), imag.astype(jnp.bfloat16)
                rows = slice(side * half_readout, (side + 1) * half_readout)
                cosine, sine = turn_s[0, part, rows], turn_s[1, part, rows]
                waved.append((real * cosine - imag * sine, real * sine + imag * cosine))
        folded = []
        for sign in (1, -1):
            sides = []
            for side in range(2):
                pieces = []
                for at in range(2):
                    low, high = waved[side][at], waved[2 + side][at]
                    pieces.append(low + high if sign > 0 else low - high)
                sides.append(pieces)
            folded.append([jnp.concatenate([sides[0][at], sides[1][at]], 0) for at in range(2)])
        return folded

    def project(folded):
        even, odd = [mxu(jnp.concatenate(folded[at], 1), table_s[at]) for at in range(2)]
        unwaved = [None] * 4
        for part, value in enumerate((even + odd, even - odd)):
            value = value.astype(jnp.bfloat16)
            real, imag = value[:, :HALF], value[:, HALF:]
            cosine, sine = turn_s[0, part], turn_s[1, part]
            unreal, unimag = real * cosine + imag * sine, imag * cosine - real * sine
            plus_real, minus_real = unreal[:half_readout], unreal[half_readout:]
            plus_imag, minus_imag = unimag[:half_readout], unimag[half_readout:]
            unwaved[part] = jnp.concatenate(
                [
                    joined(plus_real, plus_real + minus_real),
                    joined(minus_real, minus_imag - plus_imag),
                ],
                0,
            )
            unwaved[2 + part] = jnp.concatenate(
                [
                    joined(plus_imag, plus_imag + minus_imag),
                    joined(minus_imag, plus_real - minus_real),
                ],
                0,
            )
        return unwaved

    def decode(unwaved, slot):
        back = mxu(held["decode"][...], jnp.concatenate(unwaved, 1))
        for part in range(2):
            real = back[:, part * HALF : (part + 1) * HALF]
            imag = back[:, TALL + part * HALF : TALL + (part + 1) * HALF]
            coil_real, coil_imag = coil_s[slot, 0, part], coil_s[slot, 1, part]
            sum_s[0, part] += coil_real * real + coil_imag * imag
            sum_s[1, part] += coil_real * imag - coil_imag * real

    def run(start, many, entering, leaving, begin):
        if entering:
            coil_image = [coil_image_s[at] for at in range(4)]
            folded = [[fold_s[at, piece] for piece in range(2)] for at in range(2)]
            unwaved = [unwaved_s[at] for at in range(4)]
        else:
            coil_image = multiply(start, 0)
            folded = encode(coil_image)
            coil_image = multiply(start + 1, 1)
            unwaved = project(folded)
            folded = encode(coil_image)
            coil_image = multiply(start + 2, 2)
        for inner in range(many):
            decode(unwaved, (begin + inner) % UNROLL)
            if inner + 1 < many or leaving:
                unwaved = project(folded)
            if inner + 2 < many or leaving:
                folded = encode(coil_image)
            if inner + 3 < many or leaving:
                coil_image = multiply(start + inner + 3, (begin + inner + 3) % UNROLL)
        if leaving:
            for at in range(4):
                coil_image_s[at] = coil_image[at]
                unwaved_s[at] = unwaved[at]
                fold_s[at // 2, at % 2] = folded[at // 2][at % 2]

    def step(at, carry):
        run((at + 1) * UNROLL, UNROLL, True, True, 0)
        return carry

    rounds = (coils - 1) // UNROLL
    run(0, UNROLL, False, True, 0)
    if rounds > 1:
        lax.fori_loop(0, rounds - 1, step, 0)
    run(rounds * UNROLL, coils - rounds * UNROLL, True, False, 0)

    copies["column_spread"].wait()
    copies["column_back"].wait()
    real, imag = [jnp.concatenate([sum_s[at, 0], sum_s[at, 1]], 1) for at in range(2)]
    real, imag = shear_rows(real, imag, 1, -1.0)
    real, imag = shear_columns(real, imag, ("column_spread", "column_back"), -1.0)
    halves = turn_rows(real, imag, 0, -1.0)
    pl.semaphore_wait(barrier, 1)
    size = width // SPLIT
    links = []
    for at in range(SPLIT):
        span = (at * size, (at + 1) * size)
        for part in range(2):
            own_ref[part, span[0] : span[1]] = row_apply("row_back", halves[part], span)
        links.append(
            pltpu.make_async_remote_copy(
                src_ref=own_ref.at[:, pl.ds(span[0], size)],
                dst_ref=other_s.at[:, pl.ds(span[0], size)],
                send_sem=link_sems.at[2 * at],
                recv_sem=link_sems.at[2 * at + 1],
                device_id=partner,
                device_id_type=pl.DeviceIdType.MESH,
            )
        )
        links[at].start()
    for at in range(SPLIT):
        links[at].wait_recv()
    for at in range(SPLIT):
        links[at].wait_send()


def add_kernel(own_ref, other_ref, out_ref):
    height = out_ref.shape[2]
    out_ref[...] = (own_ref[...] + other_ref[...])[:, :, :height]


def whole_slice(image, coil_maps, psf_phase, line_mask, motion):
    height, width, readout = image.shape[0], image.shape[2], psf_phase.shape[1]
    coils = coil_maps.shape[0]
    arrays = {
        name: jnp.asarray(table) for name, table in host_tables(width, height, readout).items()
    }
    arrays["image"] = jnp.transpose(image, (1, 2, 0))
    arrays["coil"] = jnp.transpose(coil_maps, (0, 2, 3, 1))
    arrays["psf"] = psf_phase
    arrays["mask"] = line_mask
    arrays["motion"] = motion
    loads = [arrays[name] for name in LOADS]
    vmem = pl.BlockSpec(memory_space=pltpu.VMEM)
    anywhere = pl.BlockSpec(memory_space=pl.ANY)
    total = pl.pallas_call(
        slice_kernel,
        out_shape=[pltpu.VMEM((2, width, TALL), jnp.float32)] * 2,
        in_specs=[anywhere] * len(LOADS),
        out_specs=[vmem] * 2,
        scratch_shapes=[pltpu.SMEM(motion.shape, motion.dtype)]
        + [pltpu.VMEM(value.shape, value.dtype) for value in loads[1:]]
        + [
            pltpu.VMEM((2, width, TALL), jnp.float32),
            pltpu.VMEM((TALL, readout), jnp.float32),
            pltpu.VMEM((2, TALL, readout), jnp.bfloat16),
            pltpu.VMEM((2, width, HALF), jnp.float32),
            pltpu.VMEM((UNROLL, 2, 2, width, HALF), jnp.float32),
            pltpu.VMEM((1, TALL), jnp.float32),
            pltpu.VMEM((2, TALL, TALL), jnp.bfloat16),
            pltpu.VMEM((2, 2, readout, HALF), jnp.bfloat16),
            pltpu.VMEM((2, 2, width // 2, TALL), jnp.float32),
            pltpu.VMEM((2, 2, 8, TALL), jnp.float32),
            pltpu.VMEM((2, width, HALF), jnp.float32),
            pltpu.VMEM((2, 2, width, HALF), jnp.float32),
            pltpu.VMEM((4, width, HALF), jnp.bfloat16),
            pltpu.VMEM((2, 2, readout, HALF), jnp.bfloat16),
            pltpu.VMEM((4, readout, HALF), jnp.bfloat16),
            pltpu.VMEM((2, 2, width, HALF), jnp.float32),
            pltpu.SemaphoreType.DMA((len(LOADS),)),
            pltpu.SemaphoreType.DMA((2 * SPLIT,)),
        ],
        compiler_params=pltpu.CompilerParams(
            vmem_limit_bytes=56 * 1024 * 1024, collective_id=0, has_side_effects=True
        ),
        name="slice_kernel",
    )(*loads)
    result = pl.pallas_call(
        add_kernel,
        out_shape=jax.ShapeDtypeStruct((2, width, height), jnp.float32),
        in_specs=[vmem] * 2,
        out_specs=vmem,
        name="add_kernel",
    )(*[pltpu.with_memory_space_constraint(value, pltpu.VMEM) for value in total])
    return jnp.transpose(result, (2, 0, 1))


def on_device(image, coil_maps, psf_phase, line_mask, motion):
    lines = image.shape[0]
    width = image.shape[2]
    readout = psf_phase.shape[1]
    if lines == NY and lax.axis_size("shot") == 2 and fits(lines, width, readout):
        return whole_slice(image, coil_maps, psf_phase, line_mask, motion)
    devices = lax.axis_size("space")
    device_rank = lax.axis_index("space")
    pad_table = block(dft_parts(width, readout, readout, -1.0)).astype(jnp.bfloat16)
    crop_table = block(dft_parts(readout, width, readout, 1.0)).astype(jnp.bfloat16)
    group_size = max(1, NY // lines)
    bit_count = group_size.bit_length() - 1
    own_coils = regroup_coils(coil_maps, bit_count, device_rank)
    own_psf = gather_slice(psf_phase, bit_count, device_rank)
    projector = line_table(line_mask[0])
    rotated = rotate_shards(image, motion[0], 1, device_rank, devices)
    slab_image = gather_slice(rotated, bit_count, device_rank)
    waved = encode(own_coils, slab_image, own_psf, pad_table)
    partial_sum = decode(own_coils, project(projector, waved), own_psf, crop_table)
    combined = sum_slice(partial_sum, bit_count, device_rank)
    running = rotate_shards(combined, motion[0], -1, device_rank, devices)
    return lax.psum(running, "shot")


def solution(mesh):
    in_specs = (
        P(("parts", "space"), None, None),
        P(None, ("parts", "space"), None, None),
        P(("parts", "space"), None),
        P(("parts", "shot"), None),
        P(("parts", "shot"), None),
    )
    out_specs = P(("parts", "space"), None, None)
    return jax.shard_map(
        on_device, mesh=mesh, in_specs=in_specs, out_specs=out_specs, check_vma=False
    )
```

```python
import functools
import math

import jax
import jax.numpy as jnp
import numpy as np
from jax import lax
from jax.experimental import pallas as pl
from jax.experimental.pallas import tpu as pltpu
from jax.sharding import PartitionSpec as P

NY = 200
LEVELS = 17


PRECISE = lax.Precision.HIGHEST
ANGLE_STEP = 0.02
SHIFT_STEP = 0.5


def from_partner(value, axis, apart):
    mask = 2**apart
    pairs = [(source, source ^ mask) for source in range(lax.axis_size(axis))]
    return lax.ppermute(value, axis, pairs)


def dft_parts(size_in, size_out, modulus, sign):
    inputs = jnp.arange(size_in, dtype=jnp.int32)[:, None]
    outputs = jnp.arange(size_out, dtype=jnp.int32)[None, :]
    angle = (inputs * outputs % modulus).astype(jnp.float32) * (2.0 * jnp.pi / modulus)
    factor = float(modulus) ** (-0.5)
    return (jnp.cos(angle) * factor, jnp.sin(angle) * (sign * factor))


def block(parts):
    real_part, imag_part = parts
    upper = jnp.concatenate([real_part, imag_part], 1)
    bottom = jnp.concatenate([-imag_part, real_part], 1)
    return jnp.concatenate([upper, bottom], 0)


def quad(real_part, imag_part):
    return jnp.stack(
        [jnp.stack([real_part, -imag_part], 1), jnp.stack([imag_part, real_part], 1)], 0
    )


def signed_freq(length):
    counter = jnp.arange(length, dtype=jnp.int32)
    return jnp.where(counter < length // 2, counter, counter - length).astype(jnp.float32)


def turn_phase(values, phase):
    cosine = jnp.cos(phase)
    sine_part = jnp.sin(phase)
    real_part = values[..., 0, :]
    imag_part = values[..., 1, :]
    return jnp.stack(
        [real_part * cosine - imag_part * sine_part, real_part * sine_part + imag_part * cosine], -2
    )


def complex_mul(left, right):
    return jnp.stack(
        [
            left[..., 0, :] * right[..., 0, :] - left[..., 1, :] * right[..., 1, :],
            left[..., 0, :] * right[..., 1, :] + left[..., 1, :] * right[..., 0, :],
        ],
        -2,
    )


def conj_mul(left, right):
    return jnp.stack(
        [
            left[..., 0, :] * right[..., 0, :] + left[..., 1, :] * right[..., 1, :],
            left[..., 0, :] * right[..., 1, :] - left[..., 1, :] * right[..., 0, :],
        ],
        -2,
    )


def shear_rows(values, shift, sign):
    length = values.shape[-1]
    lines = values.shape[0]
    forward = block(dft_parts(length, length, length, -1.0))
    inverse = block(dft_parts(length, length, length, 1.0))
    spectra = jnp.dot(
        values.reshape(lines, 2 * length),
        forward,
        precision=PRECISE,
        preferred_element_type=jnp.float32,
    )
    phase = sign * -2.0 * jnp.pi / length * shift[:, None] * signed_freq(length)[None, :]
    spectra = turn_phase(spectra.reshape(lines, 2, length), phase)
    result = jnp.dot(
        spectra.reshape(lines, 2 * length),
        inverse,
        precision=PRECISE,
        preferred_element_type=jnp.float32,
    )
    return result.reshape(lines, 2, length)


def shear_columns(values, shift, sign):
    length = values.shape[1]
    forward = quad(*dft_parts(length, length, length, -1.0))
    inverse = quad(*dft_parts(length, length, length, 1.0))
    spectra = jnp.einsum("oaib,zbix->zaox", forward, values, precision=PRECISE)
    phase = sign * -2.0 * jnp.pi / length * signed_freq(length)[:, None] * shift[None, :]
    spectra = turn_phase(spectra, phase)
    return jnp.einsum("oaib,zbix->zaox", inverse, spectra, precision=PRECISE)


def geometry(motion_row):
    offsets = motion_row.astype(jnp.float32) - (LEVELS - 1) / 2.0
    angle = offsets[0] * ANGLE_STEP
    return (-jnp.tan(angle / 2.0), jnp.sin(angle), offsets[1] * SHIFT_STEP, offsets[2] * SHIFT_STEP)


def line_table(mask_row):
    cosine, sine_part = dft_parts(NY, NY, NY, 1.0)
    weight = mask_row.astype(jnp.float32)[:, None]
    real_part = jnp.dot(cosine.T, weight * cosine, precision=PRECISE) + jnp.dot(
        sine_part.T, weight * sine_part, precision=PRECISE
    )
    imag_part = jnp.dot(sine_part.T, weight * cosine, precision=PRECISE) - jnp.dot(
        cosine.T, weight * sine_part, precision=PRECISE
    )
    return quad(real_part, imag_part).astype(jnp.bfloat16)


def to_columns(values):
    return lax.all_to_all(values, "space", split_axis=2, concat_axis=0, tiled=True)


def to_rows(values):
    return lax.all_to_all(values, "space", split_axis=0, concat_axis=2, tiled=True)


def rotate_shards(values, motion_row, sign, device_rank, devices):
    slope, tilt, shift_x, shift_y = geometry(motion_row)
    lines = values.shape[0]
    width = values.shape[2]
    across = ((device_rank * lines + jnp.arange(lines, dtype=jnp.int32)) % NY).astype(
        jnp.float32
    ) - NY / 2.0

    def column_pass(current):
        columns = width // devices
        along = (device_rank * columns + jnp.arange(columns, dtype=jnp.int32)).astype(
            jnp.float32
        ) - width / 2.0
        gathered = to_columns(current)
        all_lines = gathered.shape[0]
        view_slices = gathered.reshape(all_lines // NY, NY, 2, columns)
        sheared = shear_columns(view_slices, tilt * along + shift_y, sign).reshape(
            all_lines, 2, columns
        )
        return to_rows(sheared)

    if sign > 0:
        current = shear_rows(values, slope * across + shift_x, 1.0)
        current = column_pass(current)
        return shear_rows(current, slope * across, 1.0)
    current = shear_rows(values, slope * across, -1.0)
    current = column_pass(current)
    return shear_rows(current, slope * across + shift_x, -1.0)


def gather_slice(values, bit_count, device_rank):
    for bit_index in range(bit_count):
        partner = from_partner(values, "space", bit_index)
        low_side = device_rank >> bit_index & 1 == 0
        values = jnp.where(
            low_side, jnp.concatenate([values, partner], 0), jnp.concatenate([partner, values], 0)
        )
    return values


def sum_slice(values, bit_count, device_rank):
    for bit_index in reversed(range(bit_count)):
        half_rows = values.shape[0] // 2
        low_side = device_rank >> bit_index & 1 == 0
        kept_part = jnp.where(low_side, values[:half_rows], values[half_rows:])
        sent_part = jnp.where(low_side, values[half_rows:], values[:half_rows])
        values = kept_part + from_partner(sent_part, "space", bit_index)
    return values


def regroup_coils(coil_maps, bit_count, device_rank):
    group_size = 1 << bit_count
    pieces = coil_maps.reshape((group_size, coil_maps.shape[0] // group_size) + coil_maps.shape[1:])
    for bit_index in range(bit_count):
        old_shape = pieces.shape
        halves = pieces.reshape((group_size >> bit_index + 1, 2, 1 << bit_index) + old_shape[1:])
        low_side = device_rank >> bit_index & 1 == 0
        kept_part = jnp.where(low_side, halves[:, 0], halves[:, 1])
        sent_part = jnp.where(low_side, halves[:, 1], halves[:, 0])
        partner = from_partner(sent_part, "space", bit_index)
        pieces = jnp.stack(
            [jnp.where(low_side, kept_part, partner), jnp.where(low_side, partner, kept_part)], 1
        ).reshape(old_shape)
    moved = jnp.moveaxis(pieces, 0, 1)
    return moved.reshape((moved.shape[0], group_size * coil_maps.shape[1]) + coil_maps.shape[2:])


def encode(coils, slab_image, psf_values, pad_table):
    coil_count, lines, _, width = coils.shape
    readout = psf_values.shape[1]
    coil_image = complex_mul(coils.astype(jnp.float32), slab_image[None]).astype(jnp.bfloat16)
    spectra = jnp.dot(
        coil_image.reshape(coil_count * lines, 2 * width),
        pad_table,
        preferred_element_type=jnp.float32,
    )
    return turn_phase(spectra.reshape(coil_count, lines, 2, readout), psf_values[None]).astype(
        jnp.bfloat16
    )


def project(projector, waved):
    coil_count, lines, _, columns = waved.shape
    view_slices = waved.reshape(coil_count, lines // NY, NY, 2, columns)
    projected = jnp.einsum(
        "oaib,czbik->czaok", projector, view_slices, preferred_element_type=jnp.float32
    )
    return projected.astype(jnp.bfloat16).reshape(waved.shape)


def decode(coils, projected, psf_values, crop_table):
    coil_count, lines, _, readout = projected.shape
    width = coils.shape[3]
    unwaved = turn_phase(projected.astype(jnp.float32), -psf_values[None]).astype(jnp.bfloat16)
    back = jnp.dot(
        unwaved.reshape(coil_count * lines, 2 * readout),
        crop_table,
        preferred_element_type=jnp.float32,
    )
    return jnp.sum(
        conj_mul(coils.astype(jnp.float32), back.reshape(coil_count, lines, 2, width)), 0
    )


def round_up(size, step):
    return -(-size // step) * step


HALF = 128
TALL = 2 * HALF


def fits(height, width, readout):
    return (
        height % 2 == 0
        and HALF < height
        and height // 2 < HALF
        and width % 32 == 0
        and width <= TALL
        and readout % 32 == 0
    )


def cosine_sine(rows, columns, modulus):
    turns = np.outer(rows, columns) % modulus
    angle = turns.astype(np.float64) * (2.0 * np.pi / modulus)
    return np.cos(angle), np.sin(angle)


def half_spectrum(points, modulus):
    half = modulus // 2
    cosine, sine = cosine_sine(np.arange(half), points, modulus)
    sine[0] = cosine_sine([half], points, modulus)[0][0]
    return np.concatenate([cosine, sine], 0)


def split_table(table):
    high = table.astype(np.float32).astype(jnp.bfloat16)
    low = (table - high.astype(np.float64)).astype(np.float32).astype(jnp.bfloat16)
    return np.stack([high, low])


def host_tables(width, height, readout):
    spectrum = half_spectrum(np.arange(width), readout) * readout**-0.5
    weight = np.full((width, 1), (2.0 / width) ** 0.5)
    weight[0] = weight[width // 2] = width**-0.5
    row = half_spectrum(np.arange(width), width) * weight

    middle = height // 2
    lines = np.arange(height)
    spread = np.where(lines < middle, lines, lines - middle + HALF)
    cosine, sine = cosine_sine(lines, np.arange(middle + 1), height)
    wave = np.zeros((height, TALL))
    wave[:, : middle + 1] = cosine * (2.0 / height) ** 0.5
    wave[:, 0] = height**-0.5
    wave[:, middle] = cosine[:, middle] * height**-0.5
    wave[:, HALF + 1 : HALF + middle] = sine[:, 1:middle] * (2.0 / height) ** 0.5
    natural = np.zeros((TALL, TALL))
    natural[:height] = wave
    padded = np.zeros((TALL, TALL))
    padded[spread] = wave

    cosine, sine = [part * height**-0.5 for part in cosine_sine(lines, lines, height)]
    line_left = np.zeros((HALF, 2 * TALL))
    line_left[:middle, :height] = cosine[:middle]
    line_left[:middle, TALL : TALL + height] = sine[:middle]
    line_right = np.zeros((2 * TALL, TALL))
    line_right[:height, :middle] = cosine[:, :middle]
    line_right[TALL : TALL + height, :middle] = sine[:, :middle]
    line_right[:height, HALF : HALF + middle] = sine[:, :middle]
    line_right[TALL : TALL + height, HALF : HALF + middle] = -cosine[:, :middle]

    half = readout // 2
    at = np.arange(half)
    ahead = np.zeros((half, -(-half // HALF) * HALF))
    ahead[at, at] = 1.0
    first = half // HALF * HALF
    behind = np.zeros((half, readout - first))
    behind[at, half + -at % half - first] = 1.0

    def narrow(table):
        return table.astype(np.float32).astype(jnp.bfloat16)

    return dict(
        row=split_table(row),
        row_back=split_table(row.T),
        column=split_table(natural),
        column_spread_back=split_table(padded.T),
        column_spread=split_table(padded),
        column_back=split_table(natural.T),
        ahead=narrow(ahead),
        behind=narrow(behind),
        line_left=split_table(line_left),
        line_right=split_table(line_right),
        encode=narrow(spectrum),
        decode=narrow(spectrum.T),
    )


SINE = [(-1.0) ** n / math.factorial(2 * n + 1) for n in range(6)]
COSINE = [(-1.0) ** n / math.factorial(2 * n) for n in range(7)]


def poly(square, coefficients):
    value = jnp.full_like(square, coefficients[-1])
    for coefficient in reversed(coefficients[:-1]):
        value = value * square + coefficient
    return value


def cos_sin_of_half(half):
    square = half * half
    sine = half * poly(square, SINE)
    cosine = poly(square, COSINE)
    return 1.0 - 2.0 * sine * sine, 2.0 * sine * cosine


def cos_sin_turns(turns):
    rest = turns - jnp.floor(turns + 0.5)
    return cos_sin_of_half(rest * math.pi)


def split_value(value):
    high = value.astype(jnp.bfloat16)
    return high, (value - high.astype(jnp.float32)).astype(jnp.bfloat16)


def mxu(left, right):
    return jnp.dot(left, right, preferred_element_type=jnp.float32)


def mxu_split(left, right):
    return mxu(left[0], right[0]) + (mxu(left[0], right[1]) + mxu(left[1], right[0]))


LOADS = (
    "motion",
    "psf",
    "image",
    "row",
    "row_back",
    "column",
    "column_spread_back",
    "mask",
    "ahead",
    "behind",
    "line_left",
    "line_right",
    "coil",
    "encode",
    "decode",
    "column_spread",
    "column_back",
)
EARLY = 7
LATE = 12
UNROLL = 4
SPLIT = 2


def slice_kernel(*refs):
    count = len(LOADS)
    sources = dict(zip(LOADS, refs[:count]))
    own_ref, other_s = refs[count : count + 2]
    held = dict(zip(LOADS, refs[count + 2 : 2 * count + 2]))
    (
        image_s,
        psf_s,
        wave_s,
        tail_s,
        coil_s,
        mask_s,
        table_s,
        turn_s,
        row_phase_s,
        edge_phase_s,
        column_phase_s,
        rotated_s,
        coil_image_s,
        fold_s,
        unwaved_s,
        sum_s,
        load_sems,
        link_sems,
    ) = refs[2 * count + 2 :]
    _, width, height = sources["image"].shape
    readout = sources["psf"].shape[1]
    coils = sources["coil"].shape[0]
    half_width, half_readout = width // 2, readout // 2
    tail = height - HALF
    ahead = HALF - height // 2

    copies = {
        name: pltpu.make_async_copy(sources[name], held[name], load_sems.at[at])
        for at, name in enumerate(LOADS)
    }
    for name in LOADS[:EARLY]:
        copies[name].start()
    partner = {"shot": 1 - lax.axis_index("shot")}
    barrier = pltpu.get_barrier_semaphore()
    pl.semaphore_signal(
        barrier, inc=1, device_id=partner, device_id_type=pl.DeviceIdType.MESH
    )

    image_s[...] = jnp.zeros_like(image_s)
    psf_s[...] = jnp.zeros_like(psf_s)
    tail_s[...] = jnp.zeros_like(tail_s)
    mask_s[...] = jnp.zeros_like(mask_s)
    sum_s[...] = jnp.zeros_like(sum_s)
    wave_s[...] = jnp.zeros_like(wave_s)
    copies["motion"].wait()
    motion_ref = held["motion"]
    theta = (motion_ref[0, 0].astype(jnp.float32) - (LEVELS - 1) / 2.0) * ANGLE_STEP
    shift_x = (motion_ref[0, 1].astype(jnp.float32) - (LEVELS - 1) / 2.0) * SHIFT_STEP
    shift_y = (motion_ref[0, 2].astype(jnp.float32) - (LEVELS - 1) / 2.0) * SHIFT_STEP
    half = theta * 0.5
    half_square = half * half
    slope = -half * (
        1.0
        + half_square
        * (1.0 / 3.0 + half_square * (2.0 / 15.0 + half_square * (17.0 / 315.0)))
    )
    square = theta * theta
    tilt = theta * (
        1.0 - square * (1.0 / 6.0 - square * (1.0 / 120.0 - square * (1.0 / 5040.0)))
    )

    def iota(shape, axis):
        return lax.broadcasted_iota(jnp.int32, shape, axis)

    def floats(value):
        return value.astype(jnp.float32)

    def row_phase(slot, padded, shift):
        lane = iota((8, TALL), 1)
        line = jnp.where(lane < HALF, lane, lane - ahead) if padded else lane
        distance = slope * (floats(line) - height / 2.0) + shift
        row = iota((8, TALL), 0)
        edge = distance * jnp.where(row == 0, 0.5, floats(row) * (1.0 / width))
        edge_phase_s[slot, 0], edge_phase_s[slot, 1] = cos_sin_turns(edge)
        for at in range(0, half_width, 8):
            turns = distance * (floats(row + at) * (1.0 / width))
            cosine, sine = cos_sin_turns(turns)
            row_phase_s[slot, 0, at : at + 8] = cosine
            row_phase_s[slot, 1, at : at + 8] = sine

    def column_phase():
        frequency = floats(iota((16, HALF), 1)) * (1.0 / height)
        row = iota((16, HALF), 0)
        for at in range(0, width, 16):
            turns = (tilt * (floats(row + at) - width / 2.0) + shift_y) * frequency
            cosine, sine = cos_sin_turns(turns)
            column_phase_s[0, at : at + 16] = cosine
            column_phase_s[1, at : at + 16] = sine

    def rows_of(table, part, span):
        return held[table][part] if span is None else held[table][part, span[0] : span[1]]

    def row_apply(table, value, span=None):
        return mxu_split((rows_of(table, 0, span), rows_of(table, 1, span)), value)

    def column_apply(table, value):
        return mxu_split(split_value(value), (held[table][0], held[table][1]))

    def turn_rows(real, imag, slot, sign):
        cosine, sine = row_phase_s[slot, 0], sign * row_phase_s[slot, 1]
        edge_cosine, edge_sine = edge_phase_s[slot, 0], sign * edge_phase_s[slot, 1]
        real = row_apply("row", split_value(real))
        imag = row_apply("row", split_value(imag))
        first = iota((8, TALL), 0) == 0
        even = [value[:half_width] for value in (real, imag)]
        odd = [value[half_width:] for value in (real, imag)]
        mixed = [
            jnp.where(first, -odd[1][:8], even[0][:8]),
            jnp.where(first, odd[0][:8], even[1][:8]),
        ]
        return [
            split_value(
                jnp.concatenate(
                    [
                        cosine * even[at] - sine * odd[at],
                        edge_sine * mixed[at] + edge_cosine * odd[at][:8],
                        sine[8:] * even[at][8:] + cosine[8:] * odd[at][8:],
                    ],
                    0,
                )
            )
            for at in range(2)
        ]

    def shear_rows(real, imag, slot, sign):
        real, imag = turn_rows(real, imag, slot, sign)
        return row_apply("row_back", real), row_apply("row_back", imag)

    def shear_columns(real, imag, tables, sign):
        cosine, sine = column_phase_s[0], sign * column_phase_s[1]
        real, imag = column_apply(tables[0], real), column_apply(tables[0], imag)
        even = [value[:, :HALF] for value in (real, imag)]
        odd = [value[:, HALF:] for value in (real, imag)]
        last = iota((width, HALF), 1) == height // 2
        mixed = [jnp.where(last, even[1], odd[0]), jnp.where(last, -even[0], odd[1])]
        out = []
        for at in range(2):
            out.append(
                jnp.concatenate(
                    [
                        cosine * even[at] - sine * mixed[at],
                        sine * even[at] + cosine * odd[at],
                    ],
                    1,
                )
            )
        return column_apply(tables[1], out[0]), column_apply(tables[1], out[1])

    row_phase(0, False, shift_x)
    column_phase()
    row_phase(1, True, 0.0)
    copies["psf"].wait()
    middle = height // 2
    psf_s[:middle] = held["psf"][:middle]
    psf_s[HALF : HALF + middle] = held["psf"][middle:]
    for start in (0, HALF):
        for at in range(start, start + round_up(middle, 16), 16):
            turn = cos_sin_of_half(psf_s[at : at + 16] * 0.5)
            for which in range(2):
                wave_s[which, at : at + 16] = turn[which].astype(jnp.bfloat16)
    for name in LOADS[2:EARLY]:
        copies[name].wait()
    for name in LOADS[EARLY:]:
        copies[name].start()
    image_s[:, :, :height] = held["image"][...]
    real, imag = shear_rows(image_s[0], image_s[1], 0, 1.0)
    real, imag = shear_columns(real, imag, ("column", "column_spread_back"), 1.0)

    for name in LOADS[EARLY:LATE]:
        copies[name].wait()
    for side, name in enumerate(("ahead", "behind")):
        wide = held[name].shape[1]
        for which in range(2):
            if side:
                wave = wave_s[which, :, readout - wide :]
            else:
                wave = wave_s[which, :, :wide]
            value = lax.dot_general(
                held[name][...],
                wave,
                (((1,), (1,)), ((), ())),
                preferred_element_type=jnp.float32,
            ).astype(jnp.bfloat16)
            rows = slice(side * half_readout, (side + 1) * half_readout)
            for part in range(2):
                turn_s[which, part, rows] = value[:, part * HALF : (part + 1) * HALF]

    mask_s[:, :height] = floats(held["mask"][...])
    mask = mask_s[...]
    mask = jnp.concatenate([mask, mask], 1)
    odd_line = iota(mask.shape, 1) % 2
    direct, crossed = [], []
    for parity in range(2):
        chosen = jnp.where(odd_line == parity, mask, 0.0)
        left = [
            (floats(held["line_left"][part]) * chosen).astype(jnp.bfloat16) for part in range(2)
        ]
        table = mxu_split(left, (held["line_right"][0], held["line_right"][1]))
        direct.append(table[:, :HALF])
        crossed.append(table[:, HALF:])
    diagonal = iota((HALF, HALF), 0) == iota((HALF, HALF), 1)

    def rounded(value):
        return floats(value.astype(jnp.bfloat16))

    whole = rounded(direct[0] + direct[1])
    even = rounded(whole + direct[0]) - whole
    direct = [
        jnp.where(diagonal, even, direct[0]),
        jnp.where(diagonal, whole - even, direct[1]),
    ]
    for parity in range(2):
        table_s[parity, :HALF, :HALF] = direct[parity].astype(jnp.bfloat16)
        table_s[parity, :HALF, HALF:] = crossed[parity].astype(jnp.bfloat16)
        table_s[parity, HALF:, :HALF] = (-crossed[parity]).astype(jnp.bfloat16)
        table_s[parity, HALF:, HALF:] = direct[parity].astype(jnp.bfloat16)

    real, imag = shear_rows(real, imag, 1, 1.0)
    for part in range(2):
        rotated_s[part, 0] = real[:, part * HALF : (part + 1) * HALF]
        rotated_s[part, 1] = imag[:, part * HALF : (part + 1) * HALF]


    for name in LOADS[LATE:]:
        copies[name].wait()

    def multiply(coil, slot):
        early = iota((width, HALF), 1) < ahead
        spread = []
        for at in range(2):
            low = floats(held["coil"][coil, at, :, :HALF])
            tail_s[at, :, :tail] = floats(held["coil"][coil, at, :, HALF:height])
            high = jnp.where(
                early, pltpu.roll(low, ahead, 1), pltpu.roll(tail_s[at], ahead, 1)
            )
            spread.append((low, high))
            coil_s[slot, at, 0] = low
            coil_s[slot, at, 1] = high
        reals, imags = [], []
        for part in range(2):
            real, imag = rotated_s[part, 0], rotated_s[part, 1]
            coil_real, coil_imag = spread[0][part], spread[1][part]
            reals.append((coil_real * real - coil_imag * imag).astype(jnp.bfloat16))
            imags.append((coil_real * imag + coil_imag * real).astype(jnp.bfloat16))
        return reals + imags

    first = iota((16, HALF), 0) == 0

    def joined(chosen, value):
        return jnp.concatenate([jnp.where(first, chosen[:16], value[:16]), value[16:]], 0)

    def encode(coil_image):
        spectra = mxu(held["encode"][...], jnp.concatenate(coil_image, 1))
        waved = []
        for part in range(2):
            lanes = slice(part * HALF, (part + 1) * HALF)
            even_real, even_imag = spectra[:half_readout, :TALL], spectra[:half_readout, TALL:]
            odd_real, odd_imag = spectra[half_readout:, :TALL], spectra[half_readout:, TALL:]
            even_real, even_imag = even_real[:, lanes], even_imag[:, lanes]
            odd_real, odd_imag = odd_real[:, lanes], odd_imag[:, lanes]
            sides = (
                (joined(even_real, even_real + odd_imag), joined(even_imag, even_imag - odd_real)),
                (joined(odd_real, even_real - odd_imag), joined(odd_imag, even_imag + odd_real)),
            )
            for side, (real, imag) in enumerate(sides):
                real, imag = real.astype(jnp.bfloat16), imag.astype(jnp.bfloat16)
                rows = slice(side * half_readout, (side + 1) * half_readout)
                cosine, sine = turn_s[0, part, rows], turn_s[1, part, rows]
                waved.append((real * cosine - imag * sine, real * sine + imag * cosine))
        folded = []
        for sign in (1, -1):
            sides = []
            for side in range(2):
                pieces = []
                for at in range(2):
                    low, high = waved[side][at], waved[2 + side][at]
                    pieces.append(low + high if sign > 0 else low - high)
                sides.append(pieces)
            folded.append([jnp.concatenate([sides[0][at], sides[1][at]], 0) for at in range(2)])
        return folded

    def project(folded):
        even, odd = [mxu(jnp.concatenate(folded[at], 1), table_s[at]) for at in range(2)]
        unwaved = [None] * 4
        for part, value in enumerate((even + odd, even - odd)):
            value = value.astype(jnp.bfloat16)
            real, imag = value[:, :HALF], value[:, HALF:]
            cosine, sine = turn_s[0, part], turn_s[1, part]
            unreal, unimag = real * cosine + imag * sine, imag * cosine - real * sine
            plus_real, minus_real = unreal[:half_readout], unreal[half_readout:]
            plus_imag, minus_imag = unimag[:half_readout], unimag[half_readout:]
            unwaved[part] = jnp.concatenate(
                [
                    joined(plus_real, plus_real + minus_real),
                    joined(minus_real, minus_imag - plus_imag),
                ],
                0,
            )
            unwaved[2 + part] = jnp.concatenate(
                [
                    joined(plus_imag, plus_imag + minus_imag),
                    joined(minus_imag, plus_real - minus_real),
                ],
                0,
            )
        return unwaved

    def decode(unwaved, slot):
        back = mxu(held["decode"][...], jnp.concatenate(unwaved, 1))
        for part in range(2):
            real = back[:, part * HALF : (part + 1) * HALF]
            imag = back[:, TALL + part * HALF : TALL + (part + 1) * HALF]
            coil_real, coil_imag = coil_s[slot, 0, part], coil_s[slot, 1, part]
            sum_s[0, part] += coil_real * real + coil_imag * imag
            sum_s[1, part] += coil_real * imag - coil_imag * real

    def run(start, many, entering, leaving, begin):
        if entering:
            coil_image = [coil_image_s[at] for at in range(4)]
            folded = [[fold_s[at, piece] for piece in range(2)] for at in range(2)]
            unwaved = [unwaved_s[at] for at in range(4)]
        else:
            coil_image = multiply(start, 0)
            folded = encode(coil_image)
            coil_image = multiply(start + 1, 1)
            unwaved = project(folded)
            folded = encode(coil_image)
            coil_image = multiply(start + 2, 2)
        for inner in range(many):
            old_unwaved, old_folded, old_image = unwaved, folded, coil_image
            decode(old_unwaved, (begin + inner) % UNROLL)
            if inner + 1 < many or leaving:
                unwaved = project(old_folded)
            if inner + 2 < many or leaving:
                folded = encode(old_image)
            if inner + 3 < many or leaving:
                coil_image = multiply(start + inner + 3, (begin + inner + 3) % UNROLL)
        if leaving:
            for at in range(4):
                coil_image_s[at] = coil_image[at]
                unwaved_s[at] = unwaved[at]
                fold_s[at // 2, at % 2] = folded[at // 2][at % 2]

    def step(at, carry):
        run((at + 1) * UNROLL, UNROLL, True, True, 0)
        return carry

    rounds = (coils - 1) // UNROLL
    run(0, UNROLL, False, True, 0)
    if rounds > 1:
        lax.fori_loop(0, rounds - 1, step, 0)
    run(rounds * UNROLL, coils - rounds * UNROLL, True, False, 0)

    real, imag = [jnp.concatenate([sum_s[at, 0], sum_s[at, 1]], 1) for at in range(2)]
    real, imag = shear_rows(real, imag, 1, -1.0)
    real, imag = shear_columns(real, imag, ("column_spread", "column_back"), -1.0)
    halves = turn_rows(real, imag, 0, -1.0)
    pl.semaphore_wait(barrier, 1)
    size = width // SPLIT
    links = []
    for at in range(SPLIT):
        span = (at * size, (at + 1) * size)
        for part in range(2):
            own_ref[part, span[0] : span[1]] = row_apply("row_back", halves[part], span)
        links.append(
            pltpu.make_async_remote_copy(
                src_ref=own_ref.at[:, pl.ds(span[0], size)],
                dst_ref=other_s.at[:, pl.ds(span[0], size)],
                send_sem=link_sems.at[2 * at],
                recv_sem=link_sems.at[2 * at + 1],
                device_id=partner,
                device_id_type=pl.DeviceIdType.MESH,
            )
        )
        links[at].start()
    for at in range(SPLIT):
        links[at].wait_recv()
    for at in range(SPLIT):
        links[at].wait_send()


def add_kernel(own_ref, other_ref, out_ref):
    height = out_ref.shape[2]
    out_ref[...] = (own_ref[...] + other_ref[...])[:, :, :height]


def whole_slice(image, coil_maps, psf_phase, line_mask, motion):
    height, width, readout = image.shape[0], image.shape[2], psf_phase.shape[1]
    coils = coil_maps.shape[0]
    arrays = {
        name: jnp.asarray(table) for name, table in host_tables(width, height, readout).items()
    }
    arrays["image"] = jnp.transpose(image, (1, 2, 0))
    arrays["coil"] = jnp.transpose(coil_maps, (0, 2, 3, 1))
    arrays["psf"] = psf_phase
    arrays["mask"] = line_mask
    arrays["motion"] = motion
    loads = [arrays[name] for name in LOADS]
    vmem = pl.BlockSpec(memory_space=pltpu.VMEM)
    anywhere = pl.BlockSpec(memory_space=pl.ANY)
    total = pl.pallas_call(
        slice_kernel,
        out_shape=[pltpu.VMEM((2, width, TALL), jnp.float32)] * 2,
        in_specs=[anywhere] * len(LOADS),
        out_specs=[vmem] * 2,
        scratch_shapes=[pltpu.SMEM(motion.shape, motion.dtype)]
        + [pltpu.VMEM(value.shape, value.dtype) for value in loads[1:]]
        + [
            pltpu.VMEM((2, width, TALL), jnp.float32),
            pltpu.VMEM((TALL, readout), jnp.float32),
            pltpu.VMEM((2, TALL, readout), jnp.bfloat16),
            pltpu.VMEM((2, width, HALF), jnp.float32),
            pltpu.VMEM((UNROLL, 2, 2, width, HALF), jnp.float32),
            pltpu.VMEM((1, TALL), jnp.float32),
            pltpu.VMEM((2, TALL, TALL), jnp.bfloat16),
            pltpu.VMEM((2, 2, readout, HALF), jnp.bfloat16),
            pltpu.VMEM((2, 2, width // 2, TALL), jnp.float32),
            pltpu.VMEM((2, 2, 8, TALL), jnp.float32),
            pltpu.VMEM((2, width, HALF), jnp.float32),
            pltpu.VMEM((2, 2, width, HALF), jnp.float32),
            pltpu.VMEM((4, width, HALF), jnp.bfloat16),
            pltpu.VMEM((2, 2, readout, HALF), jnp.bfloat16),
            pltpu.VMEM((4, readout, HALF), jnp.bfloat16),
            pltpu.VMEM((2, 2, width, HALF), jnp.float32),
            pltpu.SemaphoreType.DMA((len(LOADS),)),
            pltpu.SemaphoreType.DMA((2 * SPLIT,)),
        ],
        compiler_params=pltpu.CompilerParams(
            vmem_limit_bytes=56 * 1024 * 1024, collective_id=0, has_side_effects=True
        ),
        name="slice_kernel",
    )(*loads)
    result = pl.pallas_call(
        add_kernel,
        out_shape=jax.ShapeDtypeStruct((2, width, height), jnp.float32),
        in_specs=[vmem] * 2,
        out_specs=vmem,
        name="add_kernel",
    )(*[pltpu.with_memory_space_constraint(value, pltpu.VMEM) for value in total])
    return jnp.transpose(result, (2, 0, 1))


def on_device(image, coil_maps, psf_phase, line_mask, motion):
    lines = image.shape[0]
    width = image.shape[2]
    readout = psf_phase.shape[1]
    if lines == NY and lax.axis_size("shot") == 2 and fits(lines, width, readout):
        return whole_slice(image, coil_maps, psf_phase, line_mask, motion)
    devices = lax.axis_size("space")
    device_rank = lax.axis_index("space")
    pad_table = block(dft_parts(width, readout, readout, -1.0)).astype(jnp.bfloat16)
    crop_table = block(dft_parts(readout, width, readout, 1.0)).astype(jnp.bfloat16)
    group_size = max(1, NY // lines)
    bit_count = group_size.bit_length() - 1
    own_coils = regroup_coils(coil_maps, bit_count, device_rank)
    own_psf = gather_slice(psf_phase, bit_count, device_rank)
    projector = line_table(line_mask[0])
    rotated = rotate_shards(image, motion[0], 1, device_rank, devices)
    slab_image = gather_slice(rotated, bit_count, device_rank)
    waved = encode(own_coils, slab_image, own_psf, pad_table)
    partial_sum = decode(own_coils, project(projector, waved), own_psf, crop_table)
    combined = sum_slice(partial_sum, bit_count, device_rank)
    running = rotate_shards(combined, motion[0], -1, device_rank, devices)
    return lax.psum(running, "shot")


def solution(mesh):
    in_specs = (
        P(("parts", "space"), None, None),
        P(None, ("parts", "space"), None, None),
        P(("parts", "space"), None),
        P(("parts", "shot"), None),
        P(("parts", "shot"), None),
    )
    out_specs = P(("parts", "space"), None, None)
    return jax.shard_map(
        on_device, mesh=mesh, in_specs=in_specs, out_specs=out_specs, check_vma=False
    )
```

```python
import functools
import math

import jax
import jax.numpy as jnp
import numpy as np
from jax import lax
from jax.experimental import pallas as pl
from jax.experimental.pallas import tpu as pltpu
from jax.sharding import PartitionSpec as P

NY = 200
LEVELS = 17


PRECISE = lax.Precision.HIGHEST
ANGLE_STEP = 0.02
SHIFT_STEP = 0.5


def from_partner(value, axis, apart):
    mask = 2**apart
    pairs = [(source, source ^ mask) for source in range(lax.axis_size(axis))]
    return lax.ppermute(value, axis, pairs)


def dft_parts(size_in, size_out, modulus, sign):
    inputs = jnp.arange(size_in, dtype=jnp.int32)[:, None]
    outputs = jnp.arange(size_out, dtype=jnp.int32)[None, :]
    angle = (inputs * outputs % modulus).astype(jnp.float32) * (2.0 * jnp.pi / modulus)
    factor = float(modulus) ** (-0.5)
    return (jnp.cos(angle) * factor, jnp.sin(angle) * (sign * factor))


def block(parts):
    real_part, imag_part = parts
    upper = jnp.concatenate([real_part, imag_part], 1)
    bottom = jnp.concatenate([-imag_part, real_part], 1)
    return jnp.concatenate([upper, bottom], 0)


def quad(real_part, imag_part):
    return jnp.stack(
        [jnp.stack([real_part, -imag_part], 1), jnp.stack([imag_part, real_part], 1)], 0
    )


def signed_freq(length):
    counter = jnp.arange(length, dtype=jnp.int32)
    return jnp.where(counter < length // 2, counter, counter - length).astype(jnp.float32)


def turn_phase(values, phase):
    cosine = jnp.cos(phase)
    sine_part = jnp.sin(phase)
    real_part = values[..., 0, :]
    imag_part = values[..., 1, :]
    return jnp.stack(
        [real_part * cosine - imag_part * sine_part, real_part * sine_part + imag_part * cosine], -2
    )


def complex_mul(left, right):
    return jnp.stack(
        [
            left[..., 0, :] * right[..., 0, :] - left[..., 1, :] * right[..., 1, :],
            left[..., 0, :] * right[..., 1, :] + left[..., 1, :] * right[..., 0, :],
        ],
        -2,
    )


def conj_mul(left, right):
    return jnp.stack(
        [
            left[..., 0, :] * right[..., 0, :] + left[..., 1, :] * right[..., 1, :],
            left[..., 0, :] * right[..., 1, :] - left[..., 1, :] * right[..., 0, :],
        ],
        -2,
    )


def shear_rows(values, shift, sign):
    length = values.shape[-1]
    lines = values.shape[0]
    forward = block(dft_parts(length, length, length, -1.0))
    inverse = block(dft_parts(length, length, length, 1.0))
    spectra = jnp.dot(
        values.reshape(lines, 2 * length),
        forward,
        precision=PRECISE,
        preferred_element_type=jnp.float32,
    )
    phase = sign * -2.0 * jnp.pi / length * shift[:, None] * signed_freq(length)[None, :]
    spectra = turn_phase(spectra.reshape(lines, 2, length), phase)
    result = jnp.dot(
        spectra.reshape(lines, 2 * length),
        inverse,
        precision=PRECISE,
        preferred_element_type=jnp.float32,
    )
    return result.reshape(lines, 2, length)


def shear_columns(values, shift, sign):
    length = values.shape[1]
    forward = quad(*dft_parts(length, length, length, -1.0))
    inverse = quad(*dft_parts(length, length, length, 1.0))
    spectra = jnp.einsum("oaib,zbix->zaox", forward, values, precision=PRECISE)
    phase = sign * -2.0 * jnp.pi / length * signed_freq(length)[:, None] * shift[None, :]
    spectra = turn_phase(spectra, phase)
    return jnp.einsum("oaib,zbix->zaox", inverse, spectra, precision=PRECISE)


def geometry(motion_row):
    offsets = motion_row.astype(jnp.float32) - (LEVELS - 1) / 2.0
    angle = offsets[0] * ANGLE_STEP
    return (-jnp.tan(angle / 2.0), jnp.sin(angle), offsets[1] * SHIFT_STEP, offsets[2] * SHIFT_STEP)


def line_table(mask_row):
    cosine, sine_part = dft_parts(NY, NY, NY, 1.0)
    weight = mask_row.astype(jnp.float32)[:, None]
    real_part = jnp.dot(cosine.T, weight * cosine, precision=PRECISE) + jnp.dot(
        sine_part.T, weight * sine_part, precision=PRECISE
    )
    imag_part = jnp.dot(sine_part.T, weight * cosine, precision=PRECISE) - jnp.dot(
        cosine.T, weight * sine_part, precision=PRECISE
    )
    return quad(real_part, imag_part).astype(jnp.bfloat16)


def to_columns(values):
    return lax.all_to_all(values, "space", split_axis=2, concat_axis=0, tiled=True)


def to_rows(values):
    return lax.all_to_all(values, "space", split_axis=0, concat_axis=2, tiled=True)


def rotate_shards(values, motion_row, sign, device_rank, devices):
    slope, tilt, shift_x, shift_y = geometry(motion_row)
    lines = values.shape[0]
    width = values.shape[2]
    across = ((device_rank * lines + jnp.arange(lines, dtype=jnp.int32)) % NY).astype(
        jnp.float32
    ) - NY / 2.0

    def column_pass(current):
        columns = width // devices
        along = (device_rank * columns + jnp.arange(columns, dtype=jnp.int32)).astype(
            jnp.float32
        ) - width / 2.0
        gathered = to_columns(current)
        all_lines = gathered.shape[0]
        view_slices = gathered.reshape(all_lines // NY, NY, 2, columns)
        sheared = shear_columns(view_slices, tilt * along + shift_y, sign).reshape(
            all_lines, 2, columns
        )
        return to_rows(sheared)

    if sign > 0:
        current = shear_rows(values, slope * across + shift_x, 1.0)
        current = column_pass(current)
        return shear_rows(current, slope * across, 1.0)
    current = shear_rows(values, slope * across, -1.0)
    current = column_pass(current)
    return shear_rows(current, slope * across + shift_x, -1.0)


def gather_slice(values, bit_count, device_rank):
    for bit_index in range(bit_count):
        partner = from_partner(values, "space", bit_index)
        low_side = device_rank >> bit_index & 1 == 0
        values = jnp.where(
            low_side, jnp.concatenate([values, partner], 0), jnp.concatenate([partner, values], 0)
        )
    return values


def sum_slice(values, bit_count, device_rank):
    for bit_index in reversed(range(bit_count)):
        half_rows = values.shape[0] // 2
        low_side = device_rank >> bit_index & 1 == 0
        kept_part = jnp.where(low_side, values[:half_rows], values[half_rows:])
        sent_part = jnp.where(low_side, values[half_rows:], values[:half_rows])
        values = kept_part + from_partner(sent_part, "space", bit_index)
    return values


def regroup_coils(coil_maps, bit_count, device_rank):
    group_size = 1 << bit_count
    pieces = coil_maps.reshape((group_size, coil_maps.shape[0] // group_size) + coil_maps.shape[1:])
    for bit_index in range(bit_count):
        old_shape = pieces.shape
        halves = pieces.reshape((group_size >> bit_index + 1, 2, 1 << bit_index) + old_shape[1:])
        low_side = device_rank >> bit_index & 1 == 0
        kept_part = jnp.where(low_side, halves[:, 0], halves[:, 1])
        sent_part = jnp.where(low_side, halves[:, 1], halves[:, 0])
        partner = from_partner(sent_part, "space", bit_index)
        pieces = jnp.stack(
            [jnp.where(low_side, kept_part, partner), jnp.where(low_side, partner, kept_part)], 1
        ).reshape(old_shape)
    moved = jnp.moveaxis(pieces, 0, 1)
    return moved.reshape((moved.shape[0], group_size * coil_maps.shape[1]) + coil_maps.shape[2:])


def encode(coils, slab_image, psf_values, pad_table):
    coil_count, lines, _, width = coils.shape
    readout = psf_values.shape[1]
    coil_image = complex_mul(coils.astype(jnp.float32), slab_image[None]).astype(jnp.bfloat16)
    spectra = jnp.dot(
        coil_image.reshape(coil_count * lines, 2 * width),
        pad_table,
        preferred_element_type=jnp.float32,
    )
    return turn_phase(spectra.reshape(coil_count, lines, 2, readout), psf_values[None]).astype(
        jnp.bfloat16
    )


def project(projector, waved):
    coil_count, lines, _, columns = waved.shape
    view_slices = waved.reshape(coil_count, lines // NY, NY, 2, columns)
    projected = jnp.einsum(
        "oaib,czbik->czaok", projector, view_slices, preferred_element_type=jnp.float32
    )
    return projected.astype(jnp.bfloat16).reshape(waved.shape)


def decode(coils, projected, psf_values, crop_table):
    coil_count, lines, _, readout = projected.shape
    width = coils.shape[3]
    unwaved = turn_phase(projected.astype(jnp.float32), -psf_values[None]).astype(jnp.bfloat16)
    back = jnp.dot(
        unwaved.reshape(coil_count * lines, 2 * readout),
        crop_table,
        preferred_element_type=jnp.float32,
    )
    return jnp.sum(
        conj_mul(coils.astype(jnp.float32), back.reshape(coil_count, lines, 2, width)), 0
    )


def round_up(size, step):
    return -(-size // step) * step


HALF = 128
TALL = 2 * HALF


def fits(height, width, readout):
    return (
        height % 2 == 0
        and HALF < height
        and height // 2 < HALF
        and width % 32 == 0
        and width <= TALL
        and readout % 32 == 0
    )


def cosine_sine(rows, columns, modulus):
    turns = np.outer(rows, columns) % modulus
    angle = turns.astype(np.float64) * (2.0 * np.pi / modulus)
    return np.cos(angle), np.sin(angle)


def half_spectrum(points, modulus):
    half = modulus // 2
    cosine, sine = cosine_sine(np.arange(half), points, modulus)
    sine[0] = cosine_sine([half], points, modulus)[0][0]
    return np.concatenate([cosine, sine], 0)


def split_table(table):
    high = table.astype(np.float32).astype(jnp.bfloat16)
    low = (table - high.astype(np.float64)).astype(np.float32).astype(jnp.bfloat16)
    return np.stack([high, low])


def host_tables(width, height, readout):
    spectrum = half_spectrum(np.arange(width), readout) * readout**-0.5
    weight = np.full((width, 1), (2.0 / width) ** 0.5)
    weight[0] = weight[width // 2] = width**-0.5
    row = half_spectrum(np.arange(width), width) * weight

    middle = height // 2
    lines = np.arange(height)
    spread = np.where(lines < middle, lines, lines - middle + HALF)
    cosine, sine = cosine_sine(lines, np.arange(middle + 1), height)
    wave = np.zeros((height, TALL))
    wave[:, : middle + 1] = cosine * (2.0 / height) ** 0.5
    wave[:, 0] = height**-0.5
    wave[:, middle] = cosine[:, middle] * height**-0.5
    wave[:, HALF + 1 : HALF + middle] = sine[:, 1:middle] * (2.0 / height) ** 0.5
    natural = np.zeros((TALL, TALL))
    natural[:height] = wave
    padded = np.zeros((TALL, TALL))
    padded[spread] = wave

    cosine, sine = [part * height**-0.5 for part in cosine_sine(lines, lines, height)]
    line_left = np.zeros((HALF, 2 * TALL))
    line_left[:middle, :height] = cosine[:middle]
    line_left[:middle, TALL : TALL + height] = sine[:middle]
    line_right = np.zeros((2 * TALL, TALL))
    line_right[:height, :middle] = cosine[:, :middle]
    line_right[TALL : TALL + height, :middle] = sine[:, :middle]
    line_right[:height, HALF : HALF + middle] = sine[:, :middle]
    line_right[TALL : TALL + height, HALF : HALF + middle] = -cosine[:, :middle]

    half = readout // 2
    at = np.arange(half)
    ahead = np.zeros((half, -(-half // HALF) * HALF))
    ahead[at, at] = 1.0
    first = half // HALF * HALF
    behind = np.zeros((half, readout - first))
    behind[at, half + -at % half - first] = 1.0

    def narrow(table):
        return table.astype(np.float32).astype(jnp.bfloat16)

    return dict(
        row=split_table(row),
        row_back=split_table(row.T),
        column=split_table(natural),
        column_spread_back=split_table(padded.T),
        column_spread=split_table(padded),
        column_back=split_table(natural.T),
        ahead=narrow(ahead),
        behind=narrow(behind),
        line_left=split_table(line_left),
        line_right=split_table(line_right),
        encode=narrow(spectrum),
        decode=narrow(spectrum.T),
    )


SINE = [(-1.0) ** n / math.factorial(2 * n + 1) for n in range(6)]
COSINE = [(-1.0) ** n / math.factorial(2 * n) for n in range(7)]


def poly(square, coefficients):
    value = jnp.full_like(square, coefficients[-1])
    for coefficient in reversed(coefficients[:-1]):
        value = value * square + coefficient
    return value


def cos_sin_of_half(half):
    square = half * half
    sine = half * poly(square, SINE)
    cosine = poly(square, COSINE)
    return 1.0 - 2.0 * sine * sine, 2.0 * sine * cosine


def cos_sin_turns(turns):
    rest = turns - jnp.floor(turns + 0.5)
    return cos_sin_of_half(rest * math.pi)


def split_value(value):
    high = value.astype(jnp.bfloat16)
    return high, (value - high.astype(jnp.float32)).astype(jnp.bfloat16)


def mxu(left, right):
    return jnp.dot(left, right, preferred_element_type=jnp.float32)


def mxu_split(left, right):
    return mxu(left[0], right[0]) + (mxu(left[0], right[1]) + mxu(left[1], right[0]))


LOADS = (
    "motion",
    "psf",
    "image",
    "row",
    "row_back",
    "column",
    "column_spread_back",
    "mask",
    "ahead",
    "behind",
    "line_left",
    "line_right",
    "coil",
    "encode",
    "decode",
    "column_spread",
    "column_back",
)
EARLY = 7
LATE = 12
UNROLL = 4
SPLIT = 2


def slice_kernel(*refs):
    count = len(LOADS)
    sources = dict(zip(LOADS, refs[:count]))
    own_ref, other_s = refs[count : count + 2]
    held = dict(zip(LOADS, refs[count + 2 : 2 * count + 2]))
    (
        image_s,
        psf_s,
        wave_s,
        tail_s,
        coil_s,
        mask_s,
        table_s,
        turn_s,
        row_phase_s,
        edge_phase_s,
        column_phase_s,
        rotated_s,
        coil_image_s,
        fold_s,
        unwaved_s,
        sum_s,
        load_sems,
        link_sems,
    ) = refs[2 * count + 2 :]
    _, width, height = sources["image"].shape
    readout = sources["psf"].shape[1]
    coils = sources["coil"].shape[0]
    half_width, half_readout = width // 2, readout // 2
    tail = height - HALF
    ahead = HALF - height // 2

    copies = {
        name: pltpu.make_async_copy(sources[name], held[name], load_sems.at[at])
        for at, name in enumerate(LOADS)
    }
    for name in LOADS[:EARLY]:
        copies[name].start()
    partner = {"shot": 1 - lax.axis_index("shot")}
    barrier = pltpu.get_barrier_semaphore()
    pl.semaphore_signal(
        barrier, inc=1, device_id=partner, device_id_type=pl.DeviceIdType.MESH
    )

    image_s[...] = jnp.zeros_like(image_s)
    psf_s[...] = jnp.zeros_like(psf_s)
    tail_s[...] = jnp.zeros_like(tail_s)
    mask_s[...] = jnp.zeros_like(mask_s)
    sum_s[...] = jnp.zeros_like(sum_s)
    wave_s[...] = jnp.zeros_like(wave_s)
    copies["motion"].wait()
    motion_ref = held["motion"]
    theta = (motion_ref[0, 0].astype(jnp.float32) - (LEVELS - 1) / 2.0) * ANGLE_STEP
    shift_x = (motion_ref[0, 1].astype(jnp.float32) - (LEVELS - 1) / 2.0) * SHIFT_STEP
    shift_y = (motion_ref[0, 2].astype(jnp.float32) - (LEVELS - 1) / 2.0) * SHIFT_STEP
    half = theta * 0.5
    half_square = half * half
    slope = -half * (
        1.0
        + half_square
        * (1.0 / 3.0 + half_square * (2.0 / 15.0 + half_square * (17.0 / 315.0)))
    )
    square = theta * theta
    tilt = theta * (
        1.0 - square * (1.0 / 6.0 - square * (1.0 / 120.0 - square * (1.0 / 5040.0)))
    )

    def iota(shape, axis):
        return lax.broadcasted_iota(jnp.int32, shape, axis)

    def floats(value):
        return value.astype(jnp.float32)

    def row_phase(slot, padded, shift):
        lane = iota((8, TALL), 1)
        line = jnp.where(lane < HALF, lane, lane - ahead) if padded else lane
        distance = slope * (floats(line) - height / 2.0) + shift
        row = iota((8, TALL), 0)
        edge = distance * jnp.where(row == 0, 0.5, floats(row) * (1.0 / width))
        edge_phase_s[slot, 0], edge_phase_s[slot, 1] = cos_sin_turns(edge)
        for at in range(0, half_width, 8):
            turns = distance * (floats(row + at) * (1.0 / width))
            cosine, sine = cos_sin_turns(turns)
            row_phase_s[slot, 0, at : at + 8] = cosine
            row_phase_s[slot, 1, at : at + 8] = sine

    def column_phase():
        frequency = floats(iota((16, HALF), 1)) * (1.0 / height)
        row = iota((16, HALF), 0)
        for at in range(0, width, 16):
            turns = (tilt * (floats(row + at) - width / 2.0) + shift_y) * frequency
            cosine, sine = cos_sin_turns(turns)
            column_phase_s[0, at : at + 16] = cosine
            column_phase_s[1, at : at + 16] = sine

    def rows_of(table, part, span):
        return held[table][part] if span is None else held[table][part, span[0] : span[1]]

    def row_apply(table, value, span=None):
        return mxu_split((rows_of(table, 0, span), rows_of(table, 1, span)), value)

    def column_apply(table, value):
        return mxu_split(split_value(value), (held[table][0], held[table][1]))

    def turn_rows(real, imag, slot, sign):
        cosine, sine = row_phase_s[slot, 0], sign * row_phase_s[slot, 1]
        edge_cosine, edge_sine = edge_phase_s[slot, 0], sign * edge_phase_s[slot, 1]
        real = row_apply("row", split_value(real))
        imag = row_apply("row", split_value(imag))
        first = iota((8, TALL), 0) == 0
        even = [value[:half_width] for value in (real, imag)]
        odd = [value[half_width:] for value in (real, imag)]
        mixed = [
            jnp.where(first, -odd[1][:8], even[0][:8]),
            jnp.where(first, odd[0][:8], even[1][:8]),
        ]
        return [
            split_value(
                jnp.concatenate(
                    [
                        cosine * even[at] - sine * odd[at],
                        edge_sine * mixed[at] + edge_cosine * odd[at][:8],
                        sine[8:] * even[at][8:] + cosine[8:] * odd[at][8:],
                    ],
                    0,
                )
            )
            for at in range(2)
        ]

    def shear_rows(real, imag, slot, sign):
        real, imag = turn_rows(real, imag, slot, sign)
        return row_apply("row_back", real), row_apply("row_back", imag)

    def shear_columns(real, imag, tables, sign):
        cosine, sine = column_phase_s[0], sign * column_phase_s[1]
        real, imag = column_apply(tables[0], real), column_apply(tables[0], imag)
        even = [value[:, :HALF] for value in (real, imag)]
        odd = [value[:, HALF:] for value in (real, imag)]
        last = iota((width, HALF), 1) == height // 2
        mixed = [jnp.where(last, even[1], odd[0]), jnp.where(last, -even[0], odd[1])]
        out = []
        for at in range(2):
            out.append(
                jnp.concatenate(
                    [
                        cosine * even[at] - sine * mixed[at],
                        sine * even[at] + cosine * odd[at],
                    ],
                    1,
                )
            )
        return column_apply(tables[1], out[0]), column_apply(tables[1], out[1])

    row_phase(0, False, shift_x)
    column_phase()
    row_phase(1, True, 0.0)
    copies["psf"].wait()
    for name in LOADS[EARLY:]:
        copies[name].start()
    middle = height // 2
    psf_s[:middle] = held["psf"][:middle]
    psf_s[HALF : HALF + middle] = held["psf"][middle:]
    for start in (0, HALF):
        for at in range(start, start + round_up(middle, 16), 16):
            turn = cos_sin_of_half(psf_s[at : at + 16] * 0.5)
            for which in range(2):
                wave_s[which, at : at + 16] = turn[which].astype(jnp.bfloat16)
    for name in LOADS[2:EARLY]:
        copies[name].wait()
    image_s[:, :, :height] = held["image"][...]
    real, imag = shear_rows(image_s[0], image_s[1], 0, 1.0)
    real, imag = shear_columns(real, imag, ("column", "column_spread_back"), 1.0)

    for name in LOADS[EARLY:LATE]:
        copies[name].wait()
    for side, name in enumerate(("ahead", "behind")):
        wide = held[name].shape[1]
        for which in range(2):
            if side:
                wave = wave_s[which, :, readout - wide :]
            else:
                wave = wave_s[which, :, :wide]
            value = lax.dot_general(
                held[name][...],
                wave,
                (((1,), (1,)), ((), ())),
                preferred_element_type=jnp.float32,
            ).astype(jnp.bfloat16)
            rows = slice(side * half_readout, (side + 1) * half_readout)
            for part in range(2):
                turn_s[which, part, rows] = value[:, part * HALF : (part + 1) * HALF]

    mask_s[:, :height] = floats(held["mask"][...])
    mask = mask_s[...]
    mask = jnp.concatenate([mask, mask], 1)
    odd_line = iota(mask.shape, 1) % 2
    direct, crossed = [], []
    for parity in range(2):
        chosen = jnp.where(odd_line == parity, mask, 0.0)
        left = [
            (floats(held["line_left"][part]) * chosen).astype(jnp.bfloat16) for part in range(2)
        ]
        table = mxu_split(left, (held["line_right"][0], held["line_right"][1]))
        direct.append(table[:, :HALF])
        crossed.append(table[:, HALF:])
    diagonal = iota((HALF, HALF), 0) == iota((HALF, HALF), 1)

    def rounded(value):
        return floats(value.astype(jnp.bfloat16))

    whole = rounded(direct[0] + direct[1])
    even = rounded(whole + direct[0]) - whole
    direct = [
        jnp.where(diagonal, even, direct[0]),
        jnp.where(diagonal, whole - even, direct[1]),
    ]
    for parity in range(2):
        table_s[parity, :HALF, :HALF] = direct[parity].astype(jnp.bfloat16)
        table_s[parity, :HALF, HALF:] = crossed[parity].astype(jnp.bfloat16)
        table_s[parity, HALF:, :HALF] = (-crossed[parity]).astype(jnp.bfloat16)
        table_s[parity, HALF:, HALF:] = direct[parity].astype(jnp.bfloat16)

    real, imag = shear_rows(real, imag, 1, 1.0)
    for part in range(2):
        rotated_s[part, 0] = real[:, part * HALF : (part + 1) * HALF]
        rotated_s[part, 1] = imag[:, part * HALF : (part + 1) * HALF]


    for name in LOADS[LATE:]:
        copies[name].wait()

    def multiply(coil, slot):
        early = iota((width, HALF), 1) < ahead
        spread = []
        for at in range(2):
            low = floats(held["coil"][coil, at, :, :HALF])
            tail_s[at, :, :tail] = floats(held["coil"][coil, at, :, HALF:height])
            high = jnp.where(
                early, pltpu.roll(low, ahead, 1), pltpu.roll(tail_s[at], ahead, 1)
            )
            spread.append((low, high))
            coil_s[slot, at, 0] = low
            coil_s[slot, at, 1] = high
        reals, imags = [], []
        for part in range(2):
            real, imag = rotated_s[part, 0], rotated_s[part, 1]
            coil_real, coil_imag = spread[0][part], spread[1][part]
            reals.append((coil_real * real - coil_imag * imag).astype(jnp.bfloat16))
            imags.append((coil_real * imag + coil_imag * real).astype(jnp.bfloat16))
        return reals + imags

    first = iota((16, HALF), 0) == 0

    def joined(chosen, value):
        return jnp.concatenate([jnp.where(first, chosen[:16], value[:16]), value[16:]], 0)

    def encode(coil_image):
        spectra = mxu(held["encode"][...], jnp.concatenate(coil_image, 1))
        waved = []
        for part in range(2):
            lanes = slice(part * HALF, (part + 1) * HALF)
            even_real, even_imag = spectra[:half_readout, :TALL], spectra[:half_readout, TALL:]
            odd_real, odd_imag = spectra[half_readout:, :TALL], spectra[half_readout:, TALL:]
            even_real, even_imag = even_real[:, lanes], even_imag[:, lanes]
            odd_real, odd_imag = odd_real[:, lanes], odd_imag[:, lanes]
            sides = (
                (joined(even_real, even_real + odd_imag), joined(even_imag, even_imag - odd_real)),
                (joined(odd_real, even_real - odd_imag), joined(odd_imag, even_imag + odd_real)),
            )
            for side, (real, imag) in enumerate(sides):
                real, imag = real.astype(jnp.bfloat16), imag.astype(jnp.bfloat16)
                rows = slice(side * half_readout, (side + 1) * half_readout)
                cosine, sine = turn_s[0, part, rows], turn_s[1, part, rows]
                waved.append((real * cosine - imag * sine, real * sine + imag * cosine))
        folded = []
        for sign in (1, -1):
            sides = []
            for side in range(2):
                pieces = []
                for at in range(2):
                    low, high = waved[side][at], waved[2 + side][at]
                    pieces.append(low + high if sign > 0 else low - high)
                sides.append(pieces)
            folded.append([jnp.concatenate([sides[0][at], sides[1][at]], 0) for at in range(2)])
        return folded

    def project(folded):
        even, odd = [mxu(jnp.concatenate(folded[at], 1), table_s[at]) for at in range(2)]
        unwaved = [None] * 4
        for part, value in enumerate((even + odd, even - odd)):
            value = value.astype(jnp.bfloat16)
            real, imag = value[:, :HALF], value[:, HALF:]
            cosine, sine = turn_s[0, part], turn_s[1, part]
            unreal, unimag = real * cosine + imag * sine, imag * cosine - real * sine
            plus_real, minus_real = unreal[:half_readout], unreal[half_readout:]
            plus_imag, minus_imag = unimag[:half_readout], unimag[half_readout:]
            unwaved[part] = jnp.concatenate(
                [
                    joined(plus_real, plus_real + minus_real),
                    joined(minus_real, minus_imag - plus_imag),
                ],
                0,
            )
            unwaved[2 + part] = jnp.concatenate(
                [
                    joined(plus_imag, plus_imag + minus_imag),
                    joined(minus_imag, plus_real - minus_real),
                ],
                0,
            )
        return unwaved

    def decode(unwaved, slot):
        back = mxu(held["decode"][...], jnp.concatenate(unwaved, 1))
        for part in range(2):
            real = back[:, part * HALF : (part + 1) * HALF]
            imag = back[:, TALL + part * HALF : TALL + (part + 1) * HALF]
            coil_real, coil_imag = coil_s[slot, 0, part], coil_s[slot, 1, part]
            sum_s[0, part] += coil_real * real + coil_imag * imag
            sum_s[1, part] += coil_real * imag - coil_imag * real

    def run(start, many, entering, leaving, begin):
        if entering:
            coil_image = [coil_image_s[at] for at in range(4)]
            folded = [[fold_s[at, piece] for piece in range(2)] for at in range(2)]
            unwaved = [unwaved_s[at] for at in range(4)]
        else:
            coil_image = multiply(start, 0)
            folded = encode(coil_image)
            coil_image = multiply(start + 1, 1)
            unwaved = project(folded)
            folded = encode(coil_image)
            coil_image = multiply(start + 2, 2)
        for inner in range(many):
            old_unwaved, old_folded, old_image = unwaved, folded, coil_image
            decode(old_unwaved, (begin + inner) % UNROLL)
            if inner + 1 < many or leaving:
                unwaved = project(old_folded)
            if inner + 2 < many or leaving:
                folded = encode(old_image)
            if inner + 3 < many or leaving:
                coil_image = multiply(start + inner + 3, (begin + inner + 3) % UNROLL)
        if leaving:
            for at in range(4):
                coil_image_s[at] = coil_image[at]
                unwaved_s[at] = unwaved[at]
                fold_s[at // 2, at % 2] = folded[at // 2][at % 2]

    def step(at, carry):
        run((at + 1) * UNROLL, UNROLL, True, True, 0)
        return carry

    rounds = (coils - 1) // UNROLL
    run(0, UNROLL, False, True, 0)
    if rounds > 1:
        lax.fori_loop(0, rounds - 1, step, 0)
    run(rounds * UNROLL, coils - rounds * UNROLL, True, False, 0)

    real, imag = [jnp.concatenate([sum_s[at, 0], sum_s[at, 1]], 1) for at in range(2)]
    real, imag = shear_rows(real, imag, 1, -1.0)
    real, imag = shear_columns(real, imag, ("column_spread", "column_back"), -1.0)
    halves = turn_rows(real, imag, 0, -1.0)
    pl.semaphore_wait(barrier, 1)
    size = width // SPLIT
    links = []
    for at in range(SPLIT):
        span = (at * size, (at + 1) * size)
        for part in range(2):
            own_ref[part, span[0] : span[1]] = row_apply("row_back", halves[part], span)
        links.append(
            pltpu.make_async_remote_copy(
                src_ref=own_ref.at[:, pl.ds(span[0], size)],
                dst_ref=other_s.at[:, pl.ds(span[0], size)],
                send_sem=link_sems.at[2 * at],
                recv_sem=link_sems.at[2 * at + 1],
                device_id=partner,
                device_id_type=pl.DeviceIdType.MESH,
            )
        )
        links[at].start()
    for at in range(SPLIT):
        links[at].wait_recv()
    for at in range(SPLIT):
        links[at].wait_send()


def add_kernel(own_ref, other_ref, out_ref):
    height = out_ref.shape[2]
    out_ref[...] = (own_ref[...] + other_ref[...])[:, :, :height]


def whole_slice(image, coil_maps, psf_phase, line_mask, motion):
    height, width, readout = image.shape[0], image.shape[2], psf_phase.shape[1]
    coils = coil_maps.shape[0]
    arrays = {
        name: jnp.asarray(table) for name, table in host_tables(width, height, readout).items()
    }
    arrays["image"] = jnp.transpose(image, (1, 2, 0))
    arrays["coil"] = jnp.transpose(coil_maps, (0, 2, 3, 1))
    arrays["psf"] = psf_phase
    arrays["mask"] = line_mask
    arrays["motion"] = motion
    loads = [arrays[name] for name in LOADS]
    vmem = pl.BlockSpec(memory_space=pltpu.VMEM)
    anywhere = pl.BlockSpec(memory_space=pl.ANY)
    total = pl.pallas_call(
        slice_kernel,
        out_shape=[pltpu.VMEM((2, width, TALL), jnp.float32)] * 2,
        in_specs=[anywhere] * len(LOADS),
        out_specs=[vmem] * 2,
        scratch_shapes=[pltpu.SMEM(motion.shape, motion.dtype)]
        + [pltpu.VMEM(value.shape, value.dtype) for value in loads[1:]]
        + [
            pltpu.VMEM((2, width, TALL), jnp.float32),
            pltpu.VMEM((TALL, readout), jnp.float32),
            pltpu.VMEM((2, TALL, readout), jnp.bfloat16),
            pltpu.VMEM((2, width, HALF), jnp.float32),
            pltpu.VMEM((UNROLL, 2, 2, width, HALF), jnp.float32),
            pltpu.VMEM((1, TALL), jnp.float32),
            pltpu.VMEM((2, TALL, TALL), jnp.bfloat16),
            pltpu.VMEM((2, 2, readout, HALF), jnp.bfloat16),
            pltpu.VMEM((2, 2, width // 2, TALL), jnp.float32),
            pltpu.VMEM((2, 2, 8, TALL), jnp.float32),
            pltpu.VMEM((2, width, HALF), jnp.float32),
            pltpu.VMEM((2, 2, width, HALF), jnp.float32),
            pltpu.VMEM((4, width, HALF), jnp.bfloat16),
            pltpu.VMEM((2, 2, readout, HALF), jnp.bfloat16),
            pltpu.VMEM((4, readout, HALF), jnp.bfloat16),
            pltpu.VMEM((2, 2, width, HALF), jnp.float32),
            pltpu.SemaphoreType.DMA((len(LOADS),)),
            pltpu.SemaphoreType.DMA((2 * SPLIT,)),
        ],
        compiler_params=pltpu.CompilerParams(
            vmem_limit_bytes=56 * 1024 * 1024, collective_id=0, has_side_effects=True
        ),
        name="slice_kernel",
    )(*loads)
    result = pl.pallas_call(
        add_kernel,
        out_shape=jax.ShapeDtypeStruct((2, width, height), jnp.float32),
        in_specs=[vmem] * 2,
        out_specs=vmem,
        name="add_kernel",
    )(*[pltpu.with_memory_space_constraint(value, pltpu.VMEM) for value in total])
    return jnp.transpose(result, (2, 0, 1))


def on_device(image, coil_maps, psf_phase, line_mask, motion):
    lines = image.shape[0]
    width = image.shape[2]
    readout = psf_phase.shape[1]
    if lines == NY and lax.axis_size("shot") == 2 and fits(lines, width, readout):
        return whole_slice(image, coil_maps, psf_phase, line_mask, motion)
    devices = lax.axis_size("space")
    device_rank = lax.axis_index("space")
    pad_table = block(dft_parts(width, readout, readout, -1.0)).astype(jnp.bfloat16)
    crop_table = block(dft_parts(readout, width, readout, 1.0)).astype(jnp.bfloat16)
    group_size = max(1, NY // lines)
    bit_count = group_size.bit_length() - 1
    own_coils = regroup_coils(coil_maps, bit_count, device_rank)
    own_psf = gather_slice(psf_phase, bit_count, device_rank)
    projector = line_table(line_mask[0])
    rotated = rotate_shards(image, motion[0], 1, device_rank, devices)
    slab_image = gather_slice(rotated, bit_count, device_rank)
    waved = encode(own_coils, slab_image, own_psf, pad_table)
    partial_sum = decode(own_coils, project(projector, waved), own_psf, crop_table)
    combined = sum_slice(partial_sum, bit_count, device_rank)
    running = rotate_shards(combined, motion[0], -1, device_rank, devices)
    return lax.psum(running, "shot")


def solution(mesh):
    in_specs = (
        P(("parts", "space"), None, None),
        P(None, ("parts", "space"), None, None),
        P(("parts", "space"), None),
        P(("parts", "shot"), None),
        P(("parts", "shot"), None),
    )
    out_specs = P(("parts", "space"), None, None)
    return jax.shard_map(
        on_device, mesh=mesh, in_specs=in_specs, out_specs=out_specs, check_vma=False
    )
```
